256 devices in a mesh: task: 32 (over z, x_lo, core), tensor: 8 (over x_hi, y).
Axes of the slice: x: 4 (x_hi: 2, x_lo: 2; x = x_hi * 2 + x_lo), y: 4, z: 8, core: 2. Of those that a mesh axis runs over, the one named last changes fastest.
Arguments:
- inputs: bfloat16 [4096, 4096], P('task', 'tensor'), may hold values from -6 to 6
- targets: bfloat16 [4096, 4096], P('task', 'tensor'), may hold values from -6 to 6
- queries: bfloat16 [4096, 2048], P('task', 'tensor'), may hold values from -120 to 120
- key_rows: bfloat16 [4096, 2048], P('task', 'tensor'), may hold values from -4 to 4
- value_weight: bfloat16 [4096, 2048], P(None, 'tensor'), may hold values from -0.09375 to 0.09375
- output_weight: bfloat16 [2048, 4096], P('tensor'), may hold values from -0.125 to 0.125
- splits: int32 [32], P('task'), may hold values from 32 to 96
Outputs:
- meta_value: float32 [4096, 2048], P('task', 'tensor')
- meta_output: float32 [2048, 4096], P('tensor', 'task')
The draws below stay inside these ranges and needn't reach their ends.
Inputs may be any that keep to these rules, and one draw needn't show every extreme that they name: `splits`: support and query parts of every task are both nonempty.
All inputs are finite; a program needn't handle non-finite values.
Results may differ from the reference program's by a relative error of at most 0.025.
Values may be sent and summed in bfloat16 or wider, within the bound.
A program may use at most 64 MiB of HBM per device.

```python
import jax
import jax.numpy as jnp
from jax import lax

D = 4096
HD = 128
HEADS = 16
INNER = 1
TASKS_DEV = 1
TASK_LEN = 128
TOKENS = 4096
N_TASK = 32
N_TENSOR = 8


def paired(key):
    first, second = jax.random.split(jax.random.fold_in(key, 7), 2)
    query_base = jnp.clip(jax.random.normal(first, (TOKENS, HEADS * HD), jnp.float32), -4.0, 4.0)
    key_base = jnp.clip(jax.random.normal(second, (TOKENS, HEADS * HD), jnp.float32), -4.0, 4.0)
    return (query_base, key_base)


def draw_queries(key, part):
    return paired(key)[0].astype(jnp.bfloat16)


def draw_key_rows(key, part):
    return paired(key)[1].astype(jnp.bfloat16)


def touch_ends(values, own_key, smallest, high):
    extent = values.shape
    place = [jax.random.randint(jax.random.fold_in(own_key, axis), (), 0, extent[axis]) for axis in range(len(extent))]
    values = values.at[tuple(place)].set(smallest)
    longest = extent.index(max(extent))
    place[longest] = (place[longest] + 1) % extent[longest]
    return values.at[tuple(place)].set(high)


def spiked(drawn, stream_key, source, target, blocks, factor):
    def block_of(dim):
        return (jnp.arange(drawn.shape[dim]) // (drawn.shape[dim] // blocks)).reshape((-1,) + (1,) * (drawn.ndim - 1 - dim))

    one_side = jax.random.permutation(stream_key, blocks)[block_of(target)]
    second = (block_of(target) + blocks // 2) % blocks
    return jnp.where((block_of(source) == one_side) | (block_of(source) == second), factor * drawn, drawn)


def steps_of(own_key, shape, cuts, low, top_value):
    level, own = 1.0, jax.random.fold_in(own_key, 6)
    for dim, blocks in cuts:
        heights = jnp.exp(jax.random.uniform(jax.random.fold_in(own, dim), (blocks,), jnp.float32, low / len(cuts), top_value / len(cuts)))
        level = level * jnp.repeat(heights, shape[dim] // blocks).reshape([-1 if axis == dim else 1 for axis in range(len(shape))])
    return level


def bell_draw(own_key, extent, scale, reach, pieces=(), kind=jnp.bfloat16):
    array = jax.random.normal(own_key, extent, jnp.float32) * scale
    if len(pieces) > 0:
        array = steps_of(own_key, extent, pieces, -0.22, 0.18) * array
    return jnp.clip(array, min=-reach, max=reach).astype(kind)


def gaussian_with(stream_key, shape, scale, most, shards, heavy, held_as=jnp.bfloat16):
    entries = scale * jax.random.normal(stream_key, shape, jnp.float32)
    if shards:
        entries = entries * steps_of(stream_key, shape, shards, -0.22, 0.18)
    return jnp.clip(spiked(entries, jax.random.fold_in(stream_key, 3), *heavy), -most, most).astype(held_as)


def setup_inputs(seed: int = 0) -> dict:
    streams_of = jax.random.split(jax.random.key(seed), 8)
    return {
        "inputs": gaussian_with(streams_of[0], (TOKENS, D), 1.0, 6.0, ((0, 32), (1, 8)), (0, 1, 32, 2.75)),
        "targets": bell_draw(streams_of[1], (TOKENS, D), 1.0, 6.0, ((0, 32), (1, 8))),
        "queries": draw_queries(jax.random.fold_in(streams_of[7], 71), 0),
        "key_rows": draw_key_rows(jax.random.fold_in(streams_of[7], 71), 0),
        "value_weight": bell_draw(streams_of[4], (D, HEADS * HD), D ** -0.5, 0.09375, ((1, 8),)),
        "output_weight": bell_draw(streams_of[5], (HEADS * HD, D), (HEADS * HD) ** -0.5, 0.125, ((0, 8),)),
        "splits": touch_ends(jax.random.randint(streams_of[6], (TASKS_DEV * N_TASK,), TASK_LEN // 4, 3 * TASK_LEN // 4 + 1), jax.random.fold_in(streams_of[6], 1), TASK_LEN // 4, (3 * TASK_LEN // 4 + 1) - 1).astype(jnp.int32),
    }


step_rate = 0.25

def normed_rows(inputs):
    values = inputs.astype(jnp.float32)
    scale = lax.rsqrt(lax.optimization_barrier(jnp.mean(values * values, axis=-1, keepdims=True)) + 1e-05)
    return (values * scale).astype(jnp.bfloat16)

def attention_probs(queries, key_rows, heads):
    length = queries.shape[0]
    query_f = queries.astype(jnp.float32).reshape(length, heads, -1)
    key_f = key_rows.astype(jnp.float32).reshape(length, heads, -1)
    scores = jnp.einsum('ihd,jhd->hij', query_f, key_f) / jnp.sqrt(jnp.float32(query_f.shape[2]))
    position = jnp.arange(length)
    causal = position[:, None] >= position[None, :]
    scores = jnp.where(causal[None], scores, jnp.float32(-1e+30))
    scores = scores - lax.optimization_barrier(jnp.max(scores, axis=-1, keepdims=True))
    expo = jnp.exp(scores)
    return (expo / lax.optimization_barrier(jnp.sum(expo, axis=-1, keepdims=True))).astype(jnp.bfloat16)

def local_out(value_mat, output_mat, normed, probs):
    heads = probs.shape[0]
    length = normed.shape[0]
    upper = jnp.dot(normed, value_mat.astype(jnp.bfloat16), preferred_element_type=jnp.float32).astype(jnp.bfloat16)
    mixed = jnp.einsum('hij,jhd->ihd', probs.astype(jnp.float32), upper.astype(jnp.float32).reshape(length, heads, -1))
    mixed = mixed.reshape(length, -1).astype(jnp.bfloat16)
    return jnp.dot(mixed, output_mat.astype(jnp.bfloat16), preferred_element_type=jnp.float32).astype(jnp.bfloat16)

def task_meta(value_mat, output_mat, inputs, targets, queries, key_rows, split):
    cols = HEADS * HD // N_TENSOR
    group = HEADS // N_TENSOR
    normed = normed_rows(inputs)
    probs = attention_probs(queries, key_rows, HEADS)
    position = jnp.arange(TASK_LEN)
    support = (position < split).astype(jnp.float32)[:, None]
    query_mask = 1.0 - support
    count_s = split.astype(jnp.float32)
    count_q = jnp.float32(TASK_LEN) - count_s
    input_f = inputs.astype(jnp.float32)
    target_f = targets.astype(jnp.float32)

    def total(value_now, output_now):
        result = input_f
        for index in range(N_TENSOR):
            result = result + local_out(value_now[:, index * cols:(index + 1) * cols], output_now[index * cols:(index + 1) * cols], normed, probs[index * group:(index + 1) * group]).astype(jnp.float32)
        return result

    def loss(value_now, output_now, mask, count):
        error = total(value_now, output_now) - target_f
        return 0.5 * jnp.sum(mask * error * error) / count

    def meta_loss(value_now, output_now):
        for inner in range(INNER):
            grad_value, grad_output = jax.grad(loss, argnums=(0, 1))(value_now, output_now, support, count_s)
            value_now = value_now - step_rate * grad_value
            output_now = output_now - step_rate * grad_output
        return loss(value_now, output_now, query_mask, count_q)
    return jax.grad(meta_loss, argnums=(0, 1))(value_mat, output_mat)

def reference(inputs, targets, queries, key_rows, value_weight, output_weight, splits):
    count = N_TASK * TASKS_DEV
    value_f = value_weight.astype(jnp.float32)
    output_f = output_weight.astype(jnp.float32)
    items = (inputs.reshape(count, TASK_LEN, D), targets.reshape(count, TASK_LEN, D), queries.reshape(count, TASK_LEN, HEADS * HD), key_rows.reshape(count, TASK_LEN, HEADS * HD), splits.astype(jnp.int32))

    def accumulate(carry, item):
        grad_value, grad_output = task_meta(value_f, output_f, item[0], item[1], item[2], item[3], item[4])
        return ((carry[0] + grad_value, carry[1] + grad_output), None)
    start = (jnp.zeros((D, HEADS * HD), jnp.float32), jnp.zeros((HEADS * HD, D), jnp.float32))
    result, unused = lax.scan(accumulate, start, items)
    return (result[0], result[1])
```

```python
import functools

import jax
import jax.numpy as jnp
from jax import lax
from jax.experimental import pallas as pl
from jax.experimental.pallas import tpu as pltpu
from jax.sharding import PartitionSpec as P

HD = 128
TL = 128
RATE = 0.25
MESH = pl.DeviceIdType.MESH
BF = jnp.bfloat16
F32 = jnp.float32


def mm(a, b):
    return lax.dot_general(a, b, (((1,), (0,)), ((), ())), preferred_element_type=F32)


def mm_nt(a, b):
    return lax.dot_general(a, b, (((1,), (1,)), ((), ())), preferred_element_type=F32)


def mm_tn(a, b):
    return lax.dot_general(a, b, (((0,), (0,)), ((), ())), preferred_element_type=F32)


def body(
    NT, NX, NY,
    inp, tgt, qry, keyr, v_hbm, o_hbm, spl,
    out_v, out_o,
    v, xg, xn, osh, zc, fer, rs_send, rs_recv, kmat, probs,
    gvb, gob, cr_v, cr_o, xs_v, xs_o, xr_v, xr_o, zs_v, zs_o, zr_v, zr_o,
    lsem, ssem, rsem, fsem, gsem, hsem, psem, qsem,
):
    t = lax.axis_index("task")
    d = lax.axis_index("tensor")
    z, xl, c = t // 4, (t // 2) % 2, t % 2
    xh, y = d // NY, d % NY
    partner = t + 1 - 2 * c
    side = t + 2 - 4 * xl
    SH = inp.shape[1]
    steps = [(a, b) for a in range(NX) for b in range(NY)]
    order = sorted(range(1, NT), key=lambda k: -(2 * steps[k][0] + min(steps[k][1], NY - steps[k][1])))

    def peer(k, sign):
        a, b = steps[k]
        return ((xh + sign * a + NX) % NX) * NY + (y + sign * b + NY) % NY

    def send(src, dst, ss, rs, dev):
        cp = pltpu.make_async_remote_copy(src, dst, ss, rs, device_id=dev, device_id_type=MESH)
        cp.start()
        return cp

    def arrived(dst, rs):
        pltpu.make_async_remote_copy(dst, dst, ssem.at[0, 0], rs, device_id=(t, d), device_id_type=MESH).wait_recv()

    def zrot(k):
        return (z + k) % NT

    def zback(k):
        return (z + NT - k) % NT

    def drot(k):
        return (d + k) % NT

    vcopy = pltpu.make_async_copy(v_hbm, v, lsem.at[0])
    vcopy.start()
    ocopy = pltpu.make_async_copy(o_hbm.at[:, pl.ds(d * SH, SH)], osh.at[d], lsem.at[1])
    ocopy.start()

    bar = pltpu.get_barrier_semaphore()
    for k in range(1, NT):
        pl.semaphore_signal(bar, inc=1, device_id=(t, peer(k, -1)), device_id_type=MESH)
        pl.semaphore_signal(bar, inc=1, device_id=(zback(k) * 4 + xl * 2 + c, d), device_id_type=MESH)
        pl.semaphore_signal(bar, inc=1, device_id=(zback(k) * 4 + xl * 2 + c, z), device_id_type=MESH)
    pl.semaphore_signal(bar, inc=1, device_id=(partner, d), device_id_type=MESH)
    pl.semaphore_signal(bar, inc=1, device_id=(side, d), device_id_type=MESH)

    @pl.when(z != d)
    def _():
        pl.semaphore_signal(bar, inc=1, device_id=(t, z), device_id_type=MESH)

    pl.semaphore_wait(bar, 3 * (NT - 1) + 2 + jnp.where(z != d, 1, 0))

    pending = []
    for k in order:
        pending.append(send(inp, xg.at[d], ssem.at[0, k], rsem.at[0, k], (t, peer(k, 1))))
    half = pl.ds(c * HD, HD)
    other = pl.ds((1 - c) * HD, HD)
    for k in order:
        p = peer(k, 1)
        pending.append(
            send(o_hbm.at[half, pl.ds(p * SH, SH)], osh.at[d, half], ssem.at[1, k], rsem.at[1, k], (t, p))
        )

    row = lax.broadcasted_iota(jnp.int32, (TL, TL), 0)
    col = lax.broadcasted_iota(jnp.int32, (TL, TL), 1)
    for h in range(2):
        s = mm_nt(qry[:, h * HD:(h + 1) * HD], keyr[:, h * HD:(h + 1) * HD]) / jnp.sqrt(F32(HD))
        s = jnp.where(row >= col, s, F32(-1e30))
        s = s - jnp.max(s, axis=-1, keepdims=True)
        e = jnp.exp(s)
        probs[h] = (e / jnp.sum(e, axis=-1, keepdims=True)).astype(BF)

    def mix(u):
        ub = u.astype(BF)
        return jnp.concatenate([mm(probs[h], ub[:, h * HD:(h + 1) * HD]) for h in range(2)], axis=1)

    def mix_t(u):
        ub = u.astype(BF)
        return jnp.concatenate([mm_tn(probs[h], ub[:, h * HD:(h + 1) * HD]) for h in range(2)], axis=1)

    split = spl[0]
    pos = lax.broadcasted_iota(jnp.int32, (TL, 1), 0)
    sup = jnp.where(pos < split, F32(1.0), F32(0.0))
    ns = jnp.full((TL, 1), split, jnp.int32).astype(F32)
    s_w = sup / ns
    q_w = (1.0 - sup) / (F32(TL) - ns)

    a0 = inp[...].astype(F32) - tgt[...].astype(F32)
    xg[d] = inp[...]

    ss = jnp.zeros((TL, 1), F32)
    for k in [0] + order[::-1]:
        src = peer(k, -1)
        if k:
            arrived(xg.at[src], rsem.at[0, k])
        xv = xg[src].astype(F32)
        ss = ss + jnp.sum(xv * xv, axis=-1, keepdims=True)
    scale = lax.rsqrt(ss / F32(SH * NT) + F32(1e-05))
    vcopy.wait()
    u = jnp.zeros((TL, 2 * HD), F32)
    kacc = jnp.zeros((TL, TL), F32)
    for j in range(NT):
        xb = (xg[j].astype(F32) * scale).astype(BF)
        xn[j] = xb
        u = u + mm(xb, v[j * SH:(j + 1) * SH, :])
        kacc = kacc + mm_nt(xb, xb)
    kmat[...] = kacc.astype(BF)
    u = u.astype(BF).astype(F32)

    ZP, DZ, Z0 = pl.ds(0, TL), pl.ds(TL, TL), pl.ds(2 * TL, TL)

    def gather_start(part, phase):
        for k in order:
            pending.append(
                send(zc.at[d, part], zc.at[d, part], ssem.at[phase, k], rsem.at[phase, k], (t, peer(k, 1)))
            )

    zc[d, Z0, :] = mix(u).astype(BF)
    gather_start(Z0, 2)

    for k in order[::-1]:
        src = peer(k, -1)
        arrived(osh.at[src, half], rsem.at[1, k])
        pending.append(
            send(osh.at[src, half], osh.at[src, half], fsem.at[0, k], fsem.at[1, k], (partner, d))
        )
    ocopy.wait()

    def scatter(err, extra, phase, slot):
        for k in order:
            p = peer(k, 1)
            rs_send[slot, k] = (mm_nt(err, osh[p]) + extra(p)).astype(BF)
            pending.append(
                send(rs_send.at[slot, k], rs_recv.at[slot, k], ssem.at[phase, k], rsem.at[phase, k], (t, p))
            )
        return mm_nt(err, osh[d]) + extra(d)

    def scatter_end(own, phase, slot):
        acc = own
        for k in order[::-1]:
            arrived(rs_recv.at[slot, k], rsem.at[phase, k])
            acc = acc + rs_recv[slot, k].astype(F32)
        return acc

    acc = a0
    for k in [0] + order[::-1]:
        src = peer(k, -1)
        if k:
            arrived(osh.at[src, other], fsem.at[1, k])
            arrived(zc.at[src, Z0], rsem.at[2, k])
        acc = acc + mm(zc[src, Z0, :], osh[src])
    err = (acc * s_w).astype(BF)
    fer[1] = err
    own = scatter(err, lambda p: F32(0.0), 3, 0)
    dz = scatter_end(own, 3, 0)
    du = mix_t(dz)
    u2 = u - RATE * mm(kmat[...], du.astype(BF))
    zc[d, ZP, :] = mix(u2).astype(BF)
    gather_start(ZP, 4)

    acc = a0
    zz = jnp.zeros((TL, TL), F32)
    for k in [0] + order[::-1]:
        src = peer(k, -1)
        if k:
            arrived(zc.at[src, ZP], rsem.at[4, k])
        zp = zc[src, ZP, :]
        acc = acc + mm(zp, osh[src])
        zz = zz + mm_nt(zp, zc[src, Z0, :])
    zzb = (RATE * zz).astype(BF)
    acc = acc - mm(zzb, fer[1])
    qer = (acc * q_w).astype(BF)
    fer[0] = qer
    fe = (-RATE * mm_nt(qer, fer[1])).astype(BF)
    own = scatter(qer, lambda p: mm(fe, zc[p, Z0, :]), 5, 1)
    dz2 = scatter_end(own, 5, 1)
    du2 = mix_t(dz2)
    zc[d, DZ, :] = mix(-RATE * mm(kmat[...], du2.astype(BF))).astype(BF)
    gather_start(DZ, 6)

    acc = -mm_tn(zzb, fer[0])
    for k in [0] + order[::-1]:
        src = peer(k, -1)
        if k:
            arrived(zc.at[src, DZ], rsem.at[6, k])
        acc = acc + mm(zc[src, DZ, :], osh[src])
    rer = (acc * s_w).astype(BF)
    fer[2] = rer
    own = scatter(rer, lambda p: mm_tn(fe, zc[p, ZP, :]), 7, 2)

    errs = jnp.concatenate([fer[0], fer[1], fer[2]], axis=0)

    def go_step(j, carry):
        blk = mm_tn(zc[j], errs)
        for il in range(4):
            gob[il % 2, il // 2, j] = blk[:, il * HD:(il + 1) * HD].astype(BF)
        return carry

    lax.fori_loop(0, NT, go_step, 0)
    pending.append(send(gob.at[1 - c], cr_o, gsem.at[0, 0], gsem.at[1, 0], (partner, d)))

    y_in = scatter_end(own, 7, 2)
    w = mix_t(dz2 + y_in).astype(BF)

    def gv_step(j, carry):
        blk = mm_tn(xn[j], w)
        for il in range(4):
            gvb[il % 2, il // 2, j] = blk[il * TL:(il + 1) * TL, :].astype(BF)
        return carry

    lax.fori_loop(0, NT, gv_step, 0)
    pending.append(send(gvb.at[1 - c], cr_v, gsem.at[0, 1], gsem.at[1, 1], (partner, d)))

    def core_stage(g, cr, xs, xr, idx):
        arrived(cr, gsem.at[1, idx])

        def add(j, carry):
            xs[j] = (g[c, 1 - xl, j].astype(F32) + cr[1 - xl, j].astype(F32)).astype(BF)
            return carry

        lax.fori_loop(0, NT, add, 0)
        pending.append(send(xs, xr, hsem.at[0, idx], hsem.at[1, idx], (side, d)))

    core_stage(gob, cr_o, xs_o, xr_o, 0)
    core_stage(gvb, cr_v, xs_v, xr_v, 1)

    def side_stage(g, cr, xr, zs, idx):
        arrived(xr, hsem.at[1, idx])

        def add(j, carry):
            zs[j] = (g[c, xl, j].astype(F32) + cr[xl, j].astype(F32) + xr[j].astype(F32)).astype(BF)
            return carry

        lax.fori_loop(0, NT, add, 0)

    zorder = sorted(range(1, NT), key=lambda k: -min(k, NT - k))
    side_stage(gob, cr_o, xr_o, zs_o, 0)
    there = d * 4 + xl * 2 + c
    for k in zorder:
        j = drot(k)
        pending.append(send(zs_o.at[j], zr_o.at[z], psem.at[0, k], qsem.at[0, z], (there, j)))

    @pl.when(z != d)
    def _():
        send(zs_o.at[d], zr_o.at[z], psem.at[0, 0], qsem.at[0, z], (there, d)).wait_send()

    @pl.when(z == d)
    def _():
        zr_o[z] = zs_o[d]

    side_stage(gvb, cr_v, xr_v, zs_v, 1)
    for k in zorder:
        zt = zrot(k)
        pending.append(send(zs_v.at[zt], zr_v.at[k], psem.at[1, k], qsem.at[1, k], (zt * 4 + xl * 2 + c, d)))

    for k in range(1, NT):
        arrived(zr_o.at[zrot(k)], qsem.at[0, zrot(k)])

    @pl.when(z != d)
    def _():
        arrived(zr_o.at[z], qsem.at[0, z])

    acc = zr_o[0].astype(F32)
    for j in range(1, NT):
        acc = acc + zr_o[j].astype(F32)
    out_o[...] = acc

    acc = zs_v[z].astype(F32)
    for k in zorder[::-1]:
        arrived(zr_v.at[k], qsem.at[1, k])
        acc = acc + zr_v[k].astype(F32)
    out_v[...] = acc

    for cp in pending:
        cp.wait_send()


def per_device(inputs, targets, queries, key_rows, value_weight, output_weight, splits, *, NT):
    NX = 2 if NT % 8 == 0 else 1
    NY = NT // NX
    SH = inputs.shape[1]
    vm = pltpu.VMEM
    vspec = pl.BlockSpec(memory_space=pltpu.VMEM)
    aspec = pl.BlockSpec(memory_space=pl.ANY)
    dma = pltpu.SemaphoreType.DMA
    return pl.pallas_call(
        functools.partial(body, NT, NX, NY),
        out_shape=(
            jax.ShapeDtypeStruct((TL, 2 * HD), F32),
            jax.ShapeDtypeStruct((2 * HD, TL), F32),
        ),
        in_specs=[vspec] * 4 + [aspec] * 2 + [pl.BlockSpec(memory_space=pltpu.SMEM)],
        out_specs=(vspec, vspec),
        scratch_shapes=[
            vm((SH * NT, 2 * HD), BF),
            vm((NT, TL, SH), BF),
            vm((NT, TL, SH), BF),
            vm((NT, 2 * HD, SH), BF),
            vm((NT, 3 * TL, 2 * HD), BF),
            vm((3, TL, SH), BF),
            vm((3, NT, TL, 2 * HD), BF),
            vm((3, NT, TL, 2 * HD), BF),
            vm((TL, TL), BF),
            vm((2, TL, TL), BF),
            vm((2, 2, NT, TL, 2 * HD), BF),
            vm((2, 2, NT, 2 * HD, HD), BF),
            vm((2, NT, TL, 2 * HD), BF),
            vm((2, NT, 2 * HD, HD), BF),
            vm((NT, TL, 2 * HD), BF),
            vm((NT, 2 * HD, HD), BF),
            vm((NT, TL, 2 * HD), BF),
            vm((NT, 2 * HD, HD), BF),
            vm((NT, TL, 2 * HD), BF),
            vm((NT, 2 * HD, HD), BF),
            vm((NT, TL, 2 * HD), BF),
            vm((NT, 2 * HD, HD), BF),
            dma((2,)),
            dma((8, NT)),
            dma((8, NT)),
            dma((2, NT)),
            dma((2, 2)),
            dma((2, 2)),
            dma((2, NT)),
            dma((2, NT)),
        ],
        compiler_params=pltpu.CompilerParams(
            collective_id=0, has_side_effects=True, vmem_limit_bytes=60 * 1024 * 1024
        ),
        name="meta",
    )(inputs, targets, queries, key_rows, value_weight, output_weight, splits)


def solution(mesh):
    return jax.shard_map(
        functools.partial(per_device, NT=mesh.shape["tensor"]),
        mesh=mesh,
        in_specs=(
            P("task", "tensor"),
            P("task", "tensor"),
            P("task", "tensor"),
            P("task", "tensor"),
            P(None, "tensor"),
            P("tensor", None),
            P("task"),
        ),
        out_specs=(P("task", "tensor"), P("tensor", "task")),
        check_vma=False,
    )
```

```python
import functools

import jax
import jax.numpy as jnp
from jax import lax
from jax.experimental import pallas as pl
from jax.experimental.pallas import tpu as pltpu
from jax.sharding import PartitionSpec as P

HD = 128
TL = 128
RATE = 0.25
MESH = pl.DeviceIdType.MESH
BF = jnp.bfloat16
F32 = jnp.float32


def mm(a, b):
    return lax.dot_general(a, b, (((1,), (0,)), ((), ())), preferred_element_type=F32)


def mm_nt(a, b):
    return lax.dot_general(a, b, (((1,), (1,)), ((), ())), preferred_element_type=F32)


def mm_tn(a, b):
    return lax.dot_general(a, b, (((0,), (0,)), ((), ())), preferred_element_type=F32)


def body(
    NT, NX, NY,
    inp, tgt, qry, keyr, v_hbm, o_hbm, spl,
    out_v, out_o,
    v, xg, xn, osh, zc, fer, rs_send, rs_recv, kmat, probs,
    gob, cr_o, xs_o, xr_o, zs_o, zr_o, xc, wall, zs_v, zr_v,
    lsem, ssem, rsem, fsem, gsem, hsem, isem, wsem, csem, psem, qsem,
):
    t = lax.axis_index("task")
    d = lax.axis_index("tensor")
    z, xl, c = t // 4, (t // 2) % 2, t % 2
    xh, y = d // NY, d % NY
    il = xl * 2 + c
    quad_il = [il, xl * 2 + 1 - c, (1 - xl) * 2 + c, (1 - xl) * 2 + 1 - c]
    quad = [z * 4 + q for q in quad_il]
    partner, side = quad[1], quad[2]
    SH = inp.shape[1]
    steps = [(a, b) for a in range(NX) for b in range(NY)]
    order = sorted(range(1, NT), key=lambda k: -(2 * steps[k][0] + min(steps[k][1], NY - steps[k][1])))

    def peer(k, sign):
        a, b = steps[k]
        return ((xh + sign * a + NX) % NX) * NY + (y + sign * b + NY) % NY

    def send(src, dst, ss, rs, dev):
        cp = pltpu.make_async_remote_copy(src, dst, ss, rs, device_id=dev, device_id_type=MESH)
        cp.start()
        return cp

    def arrived(dst, rs):
        pltpu.make_async_remote_copy(dst, dst, ssem.at[0, 0], rs, device_id=(t, d), device_id_type=MESH).wait_recv()

    def zrot(k):
        return (z + k) % NT

    def zback(k):
        return (z + NT - k) % NT

    vcopy = pltpu.make_async_copy(v_hbm, v, lsem.at[0])
    vcopy.start()
    ocopy = pltpu.make_async_copy(o_hbm.at[:, pl.ds(d * SH, SH)], osh.at[d], lsem.at[1])
    ocopy.start()

    bar = pltpu.get_barrier_semaphore()
    greet = [(t, peer(k, -1)) for k in range(1, NT)]
    greet += [(zback(k) * 4 + il, d) for k in range(1, NT)]
    greet += [(side, peer(k, -1)) for k in range(NT)]
    greet += [(partner, d), (quad[3], d)]
    for dev in greet:
        pl.semaphore_signal(bar, inc=1, device_id=dev, device_id_type=MESH)
    pl.semaphore_wait(bar, len(greet))

    pending = []
    for k in order:
        pending.append(send(inp, xg.at[d], ssem.at[0, k], rsem.at[0, k], (t, peer(k, 1))))
    half = pl.ds(c * HD, HD)
    other = pl.ds((1 - c) * HD, HD)
    for k in order:
        p = peer(k, 1)
        pending.append(
            send(o_hbm.at[half, pl.ds(p * SH, SH)], osh.at[d, half], ssem.at[1, k], rsem.at[1, k], (t, p))
        )

    row = lax.broadcasted_iota(jnp.int32, (TL, TL), 0)
    col = lax.broadcasted_iota(jnp.int32, (TL, TL), 1)
    for h in range(2):
        s = mm_nt(qry[:, h * HD:(h + 1) * HD], keyr[:, h * HD:(h + 1) * HD]) / jnp.sqrt(F32(HD))
        s = jnp.where(row >= col, s, F32(-1e30))
        s = s - jnp.max(s, axis=-1, keepdims=True)
        e = jnp.exp(s)
        probs[h] = (e / jnp.sum(e, axis=-1, keepdims=True)).astype(BF)

    def mix(u):
        ub = u.astype(BF)
        return jnp.concatenate([mm(probs[h], ub[:, h * HD:(h + 1) * HD]) for h in range(2)], axis=1)

    def mix_t(u):
        ub = u.astype(BF)
        return jnp.concatenate([mm_tn(probs[h], ub[:, h * HD:(h + 1) * HD]) for h in range(2)], axis=1)

    split = spl[0]
    pos = lax.broadcasted_iota(jnp.int32, (TL, 1), 0)
    sup = jnp.where(pos < split, F32(1.0), F32(0.0))
    ns = jnp.full((TL, 1), split, jnp.int32).astype(F32)
    s_w = sup / ns
    q_w = (1.0 - sup) / (F32(TL) - ns)

    a0 = inp[...].astype(F32) - tgt[...].astype(F32)
    xg[d] = inp[...]

    ss = jnp.zeros((TL, 1), F32)
    for k in [0] + order[::-1]:
        src = peer(k, -1)
        if k:
            arrived(xg.at[src], rsem.at[0, k])
        xv = xg[src].astype(F32)
        ss = ss + jnp.sum(xv * xv, axis=-1, keepdims=True)
    scale = lax.rsqrt(ss / F32(SH * NT) + F32(1e-05))
    vcopy.wait()
    u = jnp.zeros((TL, 2 * HD), F32)
    kacc = jnp.zeros((TL, TL), F32)
    for j in range(NT):
        xb = (xg[j].astype(F32) * scale).astype(BF)
        xn[j] = xb
        u = u + mm(xb, v[j * SH:(j + 1) * SH, :])
        kacc = kacc + mm_nt(xb, xb)
    kmat[...] = kacc.astype(BF)
    u = u.astype(BF).astype(F32)

    ZP, DZ, Z0 = pl.ds(0, TL), pl.ds(TL, TL), pl.ds(2 * TL, TL)

    def gather_start(part, phase):
        for k in order:
            pending.append(
                send(zc.at[d, part], zc.at[d, part], ssem.at[phase, k], rsem.at[phase, k], (t, peer(k, 1)))
            )

    zc[d, Z0, :] = mix(u).astype(BF)
    gather_start(Z0, 2)

    for k in order[::-1]:
        src = peer(k, -1)
        arrived(osh.at[src, half], rsem.at[1, k])
        pending.append(
            send(osh.at[src, half], osh.at[src, half], fsem.at[0, k], fsem.at[1, k], (partner, d))
        )
    ocopy.wait()

    NC = 4 if NT % 4 == 0 else 1
    CH = NT // NC

    def columns_start(part):
        for r in range(1, 4):
            pending.append(
                send(
                    xn.at[pl.ds(part * CH, CH), :, pl.ds(quad_il[r] * HD, HD)],
                    xc.at[pl.ds(part * CH, CH), pl.ds(il * TL, TL), :],
                    csem.at[0, r, part], csem.at[1, r, part], (quad[r], d),
                )
            )

    def scatter(err, extra, phase, slot):
        for k in order:
            p = peer(k, 1)
            rs_send[slot, k] = (mm_nt(err, osh[p]) + extra(p)).astype(BF)
            pending.append(
                send(rs_send.at[slot, k], rs_recv.at[slot, k], ssem.at[phase, k], rsem.at[phase, k], (t, p))
            )
        return mm_nt(err, osh[d]) + extra(d)

    def scatter_end(own, phase, slot):
        acc = own
        for k in order[::-1]:
            arrived(rs_recv.at[slot, k], rsem.at[phase, k])
            acc = acc + rs_recv[slot, k].astype(F32)
        return acc

    acc = a0
    for k in [0] + order[::-1]:
        src = peer(k, -1)
        if k:
            arrived(osh.at[src, other], fsem.at[1, k])
            arrived(zc.at[src, Z0], rsem.at[2, k])
        acc = acc + mm(zc[src, Z0, :], osh[src])
    err = (acc * s_w).astype(BF)
    fer[1] = err
    own = scatter(err, lambda p: F32(0.0), 3, 0)
    columns_start(0)
    xc[:, pl.ds(il * TL, TL), :] = xn[:, :, pl.ds(il * HD, HD)]
    dz = scatter_end(own, 3, 0)
    du = mix_t(dz)
    u2 = u - RATE * mm(kmat[...], du.astype(BF))
    zc[d, ZP, :] = mix(u2).astype(BF)
    gather_start(ZP, 4)
    if NC > 1:
        columns_start(1)

    acc = a0
    zz = jnp.zeros((TL, TL), F32)
    for k in [0] + order[::-1]:
        src = peer(k, -1)
        if k:
            arrived(zc.at[src, ZP], rsem.at[4, k])
        zp = zc[src, ZP, :]
        acc = acc + mm(zp, osh[src])
        zz = zz + mm_nt(zp, zc[src, Z0, :])
    zzb = (RATE * zz).astype(BF)
    acc = acc - mm(zzb, fer[1])
    qer = (acc * q_w).astype(BF)
    fer[0] = qer
    fe = (-RATE * mm_nt(qer, fer[1])).astype(BF)
    own = scatter(qer, lambda p: mm(fe, zc[p, Z0, :]), 5, 1)
    if NC > 2:
        columns_start(2)
    dz2 = scatter_end(own, 5, 1)
    du2 = mix_t(dz2)
    zc[d, DZ, :] = mix(-RATE * mm(kmat[...], du2.astype(BF))).astype(BF)
    gather_start(DZ, 6)
    if NC > 3:
        columns_start(3)

    acc = -mm_tn(zzb, fer[0])
    for k in [0] + order[::-1]:
        src = peer(k, -1)
        if k:
            arrived(zc.at[src, DZ], rsem.at[6, k])
        acc = acc + mm(zc[src, DZ, :], osh[src])
    rer = (acc * s_w).astype(BF)
    fer[2] = rer
    own = scatter(rer, lambda p: mm_tn(fe, zc[p, ZP, :]), 7, 2)

    errs = jnp.concatenate([fer[0], fer[1], fer[2]], axis=0)

    def go_step(j, carry):
        blk = mm_tn(zc[j], errs)
        for q in range(4):
            gob[q % 2, q // 2, j] = blk[:, q * HD:(q + 1) * HD].astype(BF)
        send(gob.at[1 - c, :, j], cr_o.at[:, j], gsem.at[0, j], gsem.at[1, j], (partner, d))
        return carry

    lax.fori_loop(0, NT, go_step, 0)

    y_in = scatter_end(own, 7, 2)
    wall[pl.ds(il * TL, TL), :] = mix_t(dz2 + y_in).astype(BF)
    for r in (3, 2, 1):
        mine = wall.at[pl.ds(il * TL, TL), :]
        pending.append(send(mine, mine, wsem.at[0, r], wsem.at[1, r], (quad[r], d)))

    for k in order + [0]:
        j = peer(k, 1)
        arrived(cr_o.at[:, j], gsem.at[1, j])
        for rel in (1, 0):
            xt = xl + rel - 2 * rel * xl
            tot = gob[c, xt, j].astype(F32) + cr_o[xt, j].astype(F32)
            if rel == 0 and k == 0:
                xr_o[xl, d] = tot.astype(BF)
            else:
                xs_o[rel, k] = tot.astype(BF)
                pending.append(
                    send(xs_o.at[rel, k], xr_o.at[xl, d], hsem.at[rel, k], isem.at[xl, d], (z * 4 + xt * 2 + c, j))
                )

    zorder = sorted(range(1, NT), key=lambda k: -min(k, NT - k))

    def to_z(zs, zr, k, idx):
        zt = zrot(k)
        pending.append(send(zs.at[zt], zr.at[k], psem.at[idx, k], qsem.at[idx, k], (zt * 4 + il, d)))

    for part in range(NC):
        for r in range(1, 4):
            arrived(xc.at[pl.ds(part * CH, CH), pl.ds(quad_il[r] * TL, TL), :], csem.at[1, r, part])
    for r in range(1, 4):
        arrived(wall.at[pl.ds(quad_il[r] * TL, TL), :], wsem.at[1, r])
    for k in zorder:
        zt = zrot(k)
        zs_v[zt] = mm_tn(xc[zt], wall[...]).astype(BF)
        to_z(zs_v, zr_v, k, 0)
    own_v = mm_tn(xc[z], wall[...])

    for k in zorder + [0]:
        zt = zrot(k)
        for xs in range(2):

            @pl.when((xl != xs) | (d != zt))
            def _():
                arrived(xr_o.at[xs, zt], isem.at[xs, zt])

        tot = xr_o[0, zt].astype(F32) + xr_o[1, zt].astype(F32)
        if k:
            zs_o[zt] = tot.astype(BF)
            to_z(zs_o, zr_o, k, 1)
    own_o = tot

    for k in zorder[::-1]:
        arrived(zr_v.at[k], qsem.at[0, k])
        own_v = own_v + zr_v[k].astype(F32)
    out_v[...] = own_v
    for k in zorder[::-1]:
        arrived(zr_o.at[k], qsem.at[1, k])
        own_o = own_o + zr_o[k].astype(F32)
    out_o[...] = own_o

    def go_sent(j, carry):
        pltpu.make_async_remote_copy(
            gob.at[1 - c, :, j], cr_o.at[:, j], gsem.at[0, j], gsem.at[1, j],
            device_id=(partner, d), device_id_type=MESH,
        ).wait_send()
        return carry

    lax.fori_loop(0, NT, go_sent, 0)

    for cp in pending:
        cp.wait_send()


def per_device(inputs, targets, queries, key_rows, value_weight, output_weight, splits, *, NT):
    NX = 2 if NT % 8 == 0 else 1
    NY = NT // NX
    SH = inputs.shape[1]
    vm = pltpu.VMEM
    vspec = pl.BlockSpec(memory_space=pltpu.VMEM)
    aspec = pl.BlockSpec(memory_space=pl.ANY)
    dma = pltpu.SemaphoreType.DMA
    return pl.pallas_call(
        functools.partial(body, NT, NX, NY),
        out_shape=(
            jax.ShapeDtypeStruct((TL, 2 * HD), F32),
            jax.ShapeDtypeStruct((2 * HD, TL), F32),
        ),
        in_specs=[vspec] * 4 + [aspec] * 2 + [pl.BlockSpec(memory_space=pltpu.SMEM)],
        out_specs=(vspec, vspec),
        scratch_shapes=[
            vm((SH * NT, 2 * HD), BF),
            vm((NT, TL, SH), BF),
            vm((NT, TL, SH), BF),
            vm((NT, 2 * HD, SH), BF),
            vm((NT, 3 * TL, 2 * HD), BF),
            vm((3, TL, SH), BF),
            vm((3, NT, TL, 2 * HD), BF),
            vm((3, NT, TL, 2 * HD), BF),
            vm((TL, TL), BF),
            vm((2, TL, TL), BF),
            vm((2, 2, NT, 2 * HD, HD), BF),
            vm((2, NT, 2 * HD, HD), BF),
            vm((2, NT, 2 * HD, HD), BF),
            vm((2, NT, 2 * HD, HD), BF),
            vm((NT, 2 * HD, HD), BF),
            vm((NT, 2 * HD, HD), BF),
            vm((NT, 4 * TL, HD), BF),
            vm((4 * TL, 2 * HD), BF),
            vm((NT, TL, 2 * HD), BF),
            vm((NT, TL, 2 * HD), BF),
            dma((2,)),
            dma((8, NT)),
            dma((8, NT)),
            dma((2, NT)),
            dma((2, NT)),
            dma((2, NT)),
            dma((2, NT)),
            dma((2, 4)),
            dma((2, 4, 4)),
            dma((2, NT)),
            dma((2, NT)),
        ],
        compiler_params=pltpu.CompilerParams(
            collective_id=0, has_side_effects=True, vmem_limit_bytes=60 * 1024 * 1024
        ),
        name="meta",
    )(inputs, targets, queries, key_rows, value_weight, output_weight, splits)


def solution(mesh):
    return jax.shard_map(
        functools.partial(per_device, NT=mesh.shape["tensor"]),
        mesh=mesh,
        in_specs=(
            P("task", "tensor"),
            P("task", "tensor"),
            P("task", "tensor"),
            P("task", "tensor"),
            P(None, "tensor"),
            P("tensor", None),
            P("task"),
        ),
        out_specs=(P("task", "tensor"), P("tensor", "task")),
        check_vma=False,
    )
```

```python
import functools

import jax
import jax.numpy as jnp
from jax import lax
from jax.experimental import pallas as pl
from jax.experimental.pallas import tpu as pltpu
from jax.sharding import PartitionSpec as P

HD = 128
TL = 128
RATE = 0.25
MESH = pl.DeviceIdType.MESH
BF = jnp.bfloat16
F32 = jnp.float32


def mm(a, b):
    return lax.dot_general(a, b, (((1,), (0,)), ((), ())), preferred_element_type=F32)


def mm_nt(a, b):
    return lax.dot_general(a, b, (((1,), (1,)), ((), ())), preferred_element_type=F32)


def mm_tn(a, b):
    return lax.dot_general(a, b, (((0,), (0,)), ((), ())), preferred_element_type=F32)


def body(
    NT, NX, NY,
    inp_hbm, tgt_hbm, qry_hbm, key_hbm, v_hbm, o_hbm, spl,
    out_v, out_o,
    v, xg, xn, osh, zc, fer, rs_send, rs_recv, kmat, probs,
    gob, cr_o, xs_o, xr_o, zs_o, zr_o, xc, wall, zs_v, zr_v, gp_send, gp_recv, gm, tgt, qry, keyr,
    lsem, ssem, rsem, fsem, gsem, hsem, isem, wsem, csem, psem, qsem, msem, nsem, tsem,
):
    t = lax.axis_index("task")
    d = lax.axis_index("tensor")
    z, xl, c = t // 4, (t // 2) % 2, t % 2
    xh, y = d // NY, d % NY
    il = xl * 2 + c
    quad_il = [il, xl * 2 + 1 - c, (1 - xl) * 2 + c, (1 - xl) * 2 + 1 - c]
    quad = [z * 4 + q for q in quad_il]
    partner, side = quad[1], quad[2]
    SH = inp_hbm.shape[1]
    steps = [(a, b) for a in range(NX) for b in range(NY)]
    order = sorted(range(1, NT), key=lambda k: -(2 * steps[k][0] + min(steps[k][1], NY - steps[k][1])))

    def peer(k, sign):
        a, b = steps[k]
        return ((xh + sign * a + NX) % NX) * NY + (y + sign * b + NY) % NY

    def send(src, dst, ss, rs, dev):
        cp = pltpu.make_async_remote_copy(src, dst, ss, rs, device_id=dev, device_id_type=MESH)
        cp.start()
        return cp

    def arrived(dst, rs):
        pltpu.make_async_remote_copy(dst, dst, ssem.at[0, 0], rs, device_id=(t, d), device_id_type=MESH).wait_recv()

    def zrot(k):
        return (z + k) % NT

    def zback(k):
        return (z + NT - k) % NT

    loads = [
        pltpu.make_async_copy(a, b, lsem.at[2 + i])
        for i, (a, b) in enumerate([(inp_hbm, xg.at[d]), (qry_hbm, qry), (key_hbm, keyr), (tgt_hbm, tgt)])
    ]
    for cp in loads:
        cp.start()
    vcopy = pltpu.make_async_copy(v_hbm, v, lsem.at[0])
    vcopy.start()
    ocopy = pltpu.make_async_copy(o_hbm.at[:, pl.ds(d * SH, SH)], osh.at[d], lsem.at[1])
    ocopy.start()

    bar = pltpu.get_barrier_semaphore()
    greet = [(t, peer(k, -1)) for k in range(1, NT)]
    greet += [(zback(k) * 4 + il, d) for k in range(1, NT)]
    greet += [(side, peer(k, -1)) for k in range(NT)]
    greet += [(partner, d), (quad[3], d)]
    for dev in greet:
        pl.semaphore_signal(bar, inc=1, device_id=dev, device_id_type=MESH)
    pl.semaphore_wait(bar, len(greet))

    pending = []
    QR = HD // 2
    par = z % 2

    def quarter(cc, pp):
        return pl.ds(cc * HD + pp * QR, QR)

    def eighth(cc, pp, part):
        return pl.ds(cc * HD + pp * QR + part * (QR // 2), QR // 2)

    mine_q, next_q = quarter(c, par), quarter(c, 1 - par)
    for k in order:
        p = peer(k, 1)
        pending.append(
            send(o_hbm.at[mine_q, pl.ds(p * SH, SH)], osh.at[d, mine_q], ssem.at[1, k], rsem.at[1, k], (t, p))
        )
    loads[0].wait()
    for k in order:
        pending.append(send(xg.at[d], xg.at[d], ssem.at[0, k], rsem.at[0, k], (t, peer(k, 1))))
    for cp in loads[1:]:
        cp.wait()

    row = lax.broadcasted_iota(jnp.int32, (TL, TL), 0)
    col = lax.broadcasted_iota(jnp.int32, (TL, TL), 1)
    for h in range(2):
        s = mm_nt(qry[:, h * HD:(h + 1) * HD], keyr[:, h * HD:(h + 1) * HD]) / jnp.sqrt(F32(HD))
        s = jnp.where(row >= col, s, F32(-1e30))
        s = s - jnp.max(s, axis=-1, keepdims=True)
        e = jnp.exp(s)
        probs[h] = (e / jnp.sum(e, axis=-1, keepdims=True)).astype(BF)

    def mix(u):
        ub = u.astype(BF)
        return jnp.concatenate([mm(probs[h], ub[:, h * HD:(h + 1) * HD]) for h in range(2)], axis=1)

    def mix_t(u):
        ub = u.astype(BF)
        return jnp.concatenate([mm_tn(probs[h], ub[:, h * HD:(h + 1) * HD]) for h in range(2)], axis=1)

    split = spl[0]
    pos = lax.broadcasted_iota(jnp.int32, (TL, 1), 0)
    sup = jnp.where(pos < split, F32(1.0), F32(0.0))
    ns = jnp.full((TL, 1), split, jnp.int32).astype(F32)
    s_w = sup / ns
    q_w = (1.0 - sup) / (F32(TL) - ns)
    is_s = pos < split
    posr = lax.broadcasted_iota(jnp.int32, (1, TL), 1)
    q_row = jnp.where(posr < split, F32(0.0), F32(1.0)) / (F32(TL) - jnp.full((1, TL), split, jnp.int32).astype(F32))

    a0 = xg[d].astype(F32) - tgt[...].astype(F32)

    zup, zdown = (zrot(1) * 4 + il, d), (zback(1) * 4 + il, d)
    for k in order[::-1]:
        src = peer(k, -1)
        arrived(osh.at[src, mine_q], rsem.at[1, k])
        for kind, rows, dev in (
            (1, eighth(c, par, 0), zup), (2, eighth(c, par, 1), zdown), (0, mine_q, (partner, d)),
        ):
            part = osh.at[src, rows]
            pending.append(send(part, part, fsem.at[0, kind, k], fsem.at[1, kind, k], dev))
    for k in order[::-1]:
        src = peer(k, -1)
        arrived(osh.at[src, eighth(c, 1 - par, 0)], fsem.at[1, 1, k])
        arrived(osh.at[src, eighth(c, 1 - par, 1)], fsem.at[1, 2, k])
        part = osh.at[src, next_q]
        pending.append(send(part, part, fsem.at[0, 3, k], fsem.at[1, 3, k], (partner, d)))
    ss = jnp.zeros((TL, 1), F32)
    for k in [0] + order[::-1]:
        src = peer(k, -1)
        if k:
            arrived(xg.at[src], rsem.at[0, k])
        xv = xg[src].astype(F32)
        ss = ss + jnp.sum(xv * xv, axis=-1, keepdims=True)
    scale = lax.rsqrt(ss / F32(SH * NT) + F32(1e-05))
    vcopy.wait()
    u = jnp.zeros((TL, 2 * HD), F32)
    kacc = jnp.zeros((TL, TL), F32)
    for j in range(NT):
        xb = (xg[j].astype(F32) * scale).astype(BF)
        xn[j] = xb
        u = u + mm(xb, v[j * SH:(j + 1) * SH, :])
        kacc = kacc + mm_nt(xb, xb)
    kmat[...] = kacc.astype(BF)
    u = u.astype(BF).astype(F32)

    ZP, DZ, Z0 = pl.ds(0, TL), pl.ds(TL, TL), pl.ds(2 * TL, TL)

    def gather_start(part, phase):
        for k in order:
            pending.append(
                send(zc.at[d, part], zc.at[d, part], ssem.at[phase, k], rsem.at[phase, k], (t, peer(k, 1)))
            )

    zc[d, Z0, :] = mix(u).astype(BF)
    gather_start(Z0, 2)

    ocopy.wait()
    for k in order[::-1]:
        src = peer(k, -1)
        arrived(osh.at[src, quarter(1 - c, par)], fsem.at[1, 0, k])
        arrived(osh.at[src, quarter(1 - c, 1 - par)], fsem.at[1, 3, k])

    GH = NT // 2
    RI = 2 * HD // NT
    mine_g = pl.ds(c * GH, GH)
    mine_r = pl.ds(z * RI, RI)
    rows = jnp.concatenate([osh[c * GH + g, mine_r, :] for g in range(GH)], axis=0)
    for k in order:
        p = peer(k, 1)
        gp_send[k] = mm_nt(rows, osh[p]).astype(BF)
        pending.append(send(gp_send.at[k], gp_recv.at[k], ssem.at[5, k], rsem.at[5, k], (t, p)))
    gram = mm_nt(rows, osh[d])

    NC = 4 if NT % 4 == 0 else 1
    CH = NT // NC

    def columns_start(part):
        for r in range(1, 4):
            pending.append(
                send(
                    xn.at[pl.ds(part * CH, CH), :, pl.ds(quad_il[r] * HD, HD)],
                    xc.at[pl.ds(part * CH, CH), pl.ds(il * TL, TL), :],
                    csem.at[0, r, part], csem.at[1, r, part], (quad[r], d),
                )
            )

    acc = a0
    for k in [0] + order[::-1]:
        src = peer(k, -1)
        if k:
            arrived(zc.at[src, Z0], rsem.at[2, k])
        acc = acc + mm(zc[src, Z0, :], osh[src])
    err = (acc * s_w).astype(BF)
    a0b = a0.astype(BF)
    mixed = jnp.where(is_s, acc * s_w, a0).astype(BF)
    fer[1] = err
    for k in order:
        p = peer(k, 1)
        rs_send[k] = mm_nt(mixed, osh[p]).astype(BF)
        pending.append(send(rs_send.at[k], rs_recv.at[k], ssem.at[3, k], rsem.at[3, k], (t, p)))
    own = mm_nt(mixed, osh[d])
    for k in order[::-1]:
        arrived(gp_recv.at[k], rsem.at[5, k])
        gram = gram + gp_recv[k].astype(F32)
    for g in range(GH):
        gm[c * GH + g, mine_r, :] = gram[g * RI:(g + 1) * RI, :].astype(BF)
    zorder = sorted(range(1, NT), key=lambda k: -min(k, NT - k))
    for k in zorder:
        part = gm.at[mine_g, mine_r, :]
        pending.append(send(part, part, msem.at[0, k], msem.at[1, k], (zrot(k) * 4 + il, d)))
    columns_start(0)
    if NC > 1:
        columns_start(1)
    xc[:, pl.ds(il * TL, TL), :] = xn[:, :, pl.ds(il * HD, HD)]
    ea = mm_nt(err, a0b)
    ee = mm_nt(err, err)
    for k in order[::-1]:
        arrived(rs_recv.at[k], rsem.at[3, k])
        own = own + rs_recv[k].astype(F32)
    dz = jnp.where(is_s, own, F32(0.0))
    a0o = jnp.where(is_s, F32(0.0), own)
    dzb = dz.astype(BF)
    u2 = u - RATE * mm(kmat[...], mix_t(dz).astype(BF))
    z2 = mix(u2).astype(BF)
    shares = jnp.concatenate([mm_nt(dzb, z2) + ea, ee], axis=1)
    zc[d, ZP, :] = jnp.where(is_s, shares, z2.astype(F32)).astype(BF)
    gather_start(ZP, 4)
    for k in zorder:
        arrived(gm.at[mine_g, pl.ds(zback(k) * RI, RI), :], msem.at[1, k])
    pending.append(send(gm.at[mine_g], gm.at[mine_g], nsem.at[0], nsem.at[1], (partner, d)))
    arrived(gm.at[pl.ds((1 - c) * GH, GH)], nsem.at[1])

    zz = jnp.zeros((TL, TL), F32)
    tot = jnp.zeros((TL, 2 * HD), F32)
    fo = a0o
    for k in [0] + order[::-1]:
        src = peer(k, -1)
        if k:
            arrived(zc.at[src, ZP], rsem.at[4, k])
        zp = zc[src, ZP, :]
        zz = zz + mm_nt(zp, zc[src, Z0, :])
        fo = fo + mm(zp, gm[src])
        tot = tot + zp.astype(F32)
    zzb = jnp.where(is_s, F32(0.0), RATE * zz).astype(BF)
    ef = jnp.where(is_s, tot[:, :TL], F32(0.0))
    eeb = jnp.where(is_s, tot[:, TL:], F32(0.0)).astype(BF)
    fet = (-RATE * q_row * (ef - mm_nt(eeb, zzb))).astype(BF)
    fo = q_w * (fo - mm(zzb, dzb))
    dz2 = fo + mm_tn(fet, zc[d, Z0, :])
    zc[d, DZ, :] = mix(-RATE * mm(kmat[...], mix_t(dz2).astype(BF))).astype(BF)
    gather_start(DZ, 6)
    for part in range(2, NC):
        columns_start(part)
    acc = a0 - mm(zzb, fer[1])
    for j in range(NT):
        acc = acc + mm(zc[j, ZP, :], osh[j])
    fer[0] = (acc * q_w).astype(BF)
    acc = -mm_tn(zzb, fer[0])
    y_in = -mm_tn(zzb, fo.astype(BF))
    y_fix = mm(fet, z2)
    for k in [0] + order[::-1]:
        src = peer(k, -1)
        if k:
            arrived(zc.at[src, DZ], rsem.at[6, k])
        y_in = y_in + mm(zc[src, DZ, :], gm[src])
        acc = acc + mm(zc[src, DZ, :], osh[src])
    wall[pl.ds(il * TL, TL), :] = mix_t(dz2 + s_w * y_in + y_fix).astype(BF)
    for r in (2, 1):
        mine = wall.at[pl.ds(il * TL, TL), :]
        pending.append(send(mine, mine, wsem.at[0, r], wsem.at[1, r], (quad[r], d)))

    fer[2] = (acc * s_w).astype(BF)
    errs = jnp.concatenate([fer[0], fer[1], fer[2]], axis=0)
    todo = order + [0]
    LAG = 3
    for i in range(NT + LAG):
        if i < NT:
            j = peer(todo[i], 1)
            blk = mm_tn(zc[j], errs)
            for q in range(4):
                gob[q % 2, q // 2, j] = blk[:, q * HD:(q + 1) * HD].astype(BF)
            pending.append(
                send(gob.at[1 - c, :, j], cr_o.at[:, j], gsem.at[0, todo[i]], gsem.at[1, todo[i]], (partner, d))
            )
        if i >= LAG:
            k = todo[i - LAG]
            j = peer(k, 1)
            arrived(cr_o.at[:, j], gsem.at[1, k])
            for rel in (1, 0):
                xt = xl + rel - 2 * rel * xl
                tot = gob[c, xt, j].astype(F32) + cr_o[xt, j].astype(F32)
                if rel == 0 and k == 0:
                    xr_o[xl, d] = tot.astype(BF)
                else:
                    xs_o[rel, k] = tot.astype(BF)
                    pending.append(
                        send(xs_o.at[rel, k], xr_o.at[xl, d], hsem.at[rel, k], isem.at[xl, d], (z * 4 + xt * 2 + c, j))
                    )

    for part in range(NC):
        for r in range(1, 4):
            arrived(xc.at[pl.ds(part * CH, CH), pl.ds(quad_il[r] * TL, TL), :], csem.at[1, r, part])
    theirs = wall.at[pl.ds(quad_il[2] * TL, TL), :]
    arrived(theirs, wsem.at[1, 2])
    pending.append(send(theirs, theirs, wsem.at[0, 3], wsem.at[1, 3], (partner, d)))
    for r in (1, 3):
        arrived(wall.at[pl.ds(quad_il[r] * TL, TL), :], wsem.at[1, r])
    DN = NT // 2
    UP = NT - 1 - DN

    def v_block(zt):
        return mm_tn(xc[zt], wall[...])

    def ring(way, hop, total):
        to = zback(1) if way == 0 else zrot(1)
        zs_v[way, hop] = total.astype(BF)
        pending.append(
            send(
                zs_v.at[way, hop], zr_v.at[way, hop], psem.at[way, hop], qsem.at[way, hop], (to * 4 + il, d)
            )
        )

    def ring_first():
        ring(0, 0, v_block(zback(DN)))
        if UP:
            ring(1, 0, v_block(zrot(UP)))

    def ring_next(hop):
        for way, count in ((0, DN), (1, UP)):
            if hop < count:
                blk = v_block(zback(DN - hop) if way == 0 else zrot(UP - hop))
                arrived(zr_v.at[way, hop - 1], qsem.at[way, hop - 1])
                ring(way, hop, blk + zr_v[way, hop - 1].astype(F32))

    def plane_o(k):
        zt = zrot(k)
        for xs in range(2):

            @pl.when((xl != xs) | (d != zt))
            def _():
                arrived(xr_o.at[xs, zt], isem.at[xs, zt])

        tot = xr_o[0, zt].astype(F32) + xr_o[1, zt].astype(F32)
        if k:
            zs_o[k] = tot.astype(BF)
            pending.append(send(zs_o.at[k], zr_o.at[k], tsem.at[0, k], tsem.at[1, k], (zt * 4 + il, d)))
        return tot

    ring_first()
    for hop in range(1, DN - 1):
        ring_next(hop)
    for k in zorder + [0]:
        own_o = plane_o(k)
    if DN > 1:
        ring_next(DN - 1)
    own_v = v_block(z)
    for way, count in ((0, DN), (1, UP)):
        if count:
            arrived(zr_v.at[way, count - 1], qsem.at[way, count - 1])
            own_v = own_v + zr_v[way, count - 1].astype(F32)
    out_v[...] = own_v
    for k in zorder[::-1]:
        arrived(zr_o.at[k], tsem.at[1, k])
        own_o = own_o + zr_o[k].astype(F32)
    out_o[...] = own_o

    for cp in pending:
        cp.wait_send()


def finish(a_ref, b_ref, out_v, out_o):
    out_v[...] = a_ref[...]
    out_o[...] = b_ref[...]


def per_device(inputs, targets, queries, key_rows, value_weight, output_weight, splits, *, NT):
    NX = 2 if NT % 8 == 0 else 1
    NY = NT // NX
    SH = inputs.shape[1]
    vm = pltpu.VMEM
    vspec = pl.BlockSpec(memory_space=pltpu.VMEM)
    aspec = pl.BlockSpec(memory_space=pl.ANY)
    dma = pltpu.SemaphoreType.DMA
    parts = pl.pallas_call(
        functools.partial(body, NT, NX, NY),
        out_shape=(
            jax.ShapeDtypeStruct((TL, 2 * HD), F32),
            jax.ShapeDtypeStruct((2 * HD, TL), F32),
        ),
        in_specs=[aspec] * 6 + [pl.BlockSpec(memory_space=pltpu.SMEM)],
        out_specs=(vspec, vspec),
        scratch_shapes=[
            vm((SH * NT, 2 * HD), BF),
            vm((NT, TL, SH), BF),
            vm((NT, TL, SH), BF),
            vm((NT, 2 * HD, SH), BF),
            vm((NT, 3 * TL, 2 * HD), BF),
            vm((3, TL, SH), BF),
            vm((NT, TL, 2 * HD), BF),
            vm((NT, TL, 2 * HD), BF),
            vm((TL, TL), BF),
            vm((2, TL, TL), BF),
            vm((2, 2, NT, 2 * HD, HD), BF),
            vm((2, NT, 2 * HD, HD), BF),
            vm((2, NT, 2 * HD, HD), BF),
            vm((2, NT, 2 * HD, HD), BF),
            vm((NT, 2 * HD, HD), BF),
            vm((NT, 2 * HD, HD), BF),
            vm((NT, 4 * TL, HD), BF),
            vm((4 * TL, 2 * HD), BF),
            vm((2, NT // 2, TL, 2 * HD), BF),
            vm((2, NT // 2, TL, 2 * HD), BF),
            vm((NT, TL, 2 * HD), BF),
            vm((NT, TL, 2 * HD), BF),
            vm((NT, 2 * HD, 2 * HD), BF),
            vm((TL, SH), BF),
            vm((TL, 2 * HD), BF),
            vm((TL, 2 * HD), BF),
            dma((6,)),
            dma((8, NT)),
            dma((8, NT)),
            dma((2, 4, NT)),
            dma((2, NT)),
            dma((2, NT)),
            dma((2, NT)),
            dma((2, 4)),
            dma((2, 4, 4)),
            dma((2, NT)),
            dma((2, NT)),
            dma((2, NT)),
            dma((2,)),
            dma((2, NT)),
        ],
        compiler_params=pltpu.CompilerParams(
            collective_id=0, has_side_effects=True, vmem_limit_bytes=60 * 1024 * 1024
        ),
        name="meta",
    )(inputs, targets, queries, key_rows, value_weight, output_weight, splits)
    return pl.pallas_call(
        finish,
        out_shape=(
            jax.ShapeDtypeStruct((TL, 2 * HD), F32),
            jax.ShapeDtypeStruct((2 * HD, TL), F32),
        ),
        in_specs=[vspec] * 2,
        out_specs=(vspec, vspec),
        name="finish",
    )(*parts)


def solution(mesh):
    return jax.shard_map(
        functools.partial(per_device, NT=mesh.shape["tensor"]),
        mesh=mesh,
        in_specs=(
            P("task", "tensor"),
            P("task", "tensor"),
            P("task", "tensor"),
            P("task", "tensor"),
            P(None, "tensor"),
            P("tensor", None),
            P("task"),
        ),
        out_specs=(P("task", "tensor"), P("tensor", "task")),
        check_vma=False,
    )
```

```python
import functools

import jax
import jax.numpy as jnp
from jax import lax
from jax.experimental import pallas as pl
from jax.experimental.pallas import tpu as pltpu
from jax.sharding import PartitionSpec as P

HD = 128
TL = 128
RATE = 0.25
PH = 2
MESH = pl.DeviceIdType.MESH
BF = jnp.bfloat16
F32 = jnp.float32


def mm(a, b):
    return lax.dot_general(a, b, (((1,), (0,)), ((), ())), preferred_element_type=F32)


def mm_nt(a, b):
    return lax.dot_general(a, b, (((1,), (1,)), ((), ())), preferred_element_type=F32)


def mm_tn(a, b):
    return lax.dot_general(a, b, (((0,), (0,)), ((), ())), preferred_element_type=F32)


def body(
    NT, NX, NY,
    inp_hbm, tgt_hbm, qry_hbm, key_hbm, v_hbm, o_hbm, spl,
    out_v, out_o,
    v, xg, xn, osh, zc, fer, rs_send, rs_recv, kmat, probs,
    gob, cr_o, xs_o, xr_o, zs_o, zr_o, xc, wall, zs_v, zr_v, gp_send, gp_recv, gm, tgt, qry, keyr,
    lsem, ssem, rsem, fsem, gsem, hsem, isem, wsem, csem, psem, qsem, msem, nsem, tsem,
):
    t = lax.axis_index("task")
    d = lax.axis_index("tensor")
    z, xl, c = t // 4, (t // 2) % 2, t % 2
    xh, y = d // NY, d % NY
    il = xl * 2 + c
    quad_il = [il, xl * 2 + 1 - c, (1 - xl) * 2 + c, (1 - xl) * 2 + 1 - c]
    quad = [z * 4 + q for q in quad_il]
    partner, side = quad[1], quad[2]
    SH = inp_hbm.shape[1]
    steps = [(a, b) for a in range(NX) for b in range(NY)]
    order = sorted(range(1, NT), key=lambda k: -(2 * steps[k][0] + min(steps[k][1], NY - steps[k][1])))

    def peer(k, sign):
        a, b = steps[k]
        return ((xh + sign * a + NX) % NX) * NY + (y + sign * b + NY) % NY

    def send(src, dst, ss, rs, dev):
        cp = pltpu.make_async_remote_copy(src, dst, ss, rs, device_id=dev, device_id_type=MESH)
        cp.start()
        return cp

    def arrived(dst, rs):
        pltpu.make_async_remote_copy(dst, dst, ssem.at[0, 0], rs, device_id=(t, d), device_id_type=MESH).wait_recv()

    def sent(size, ss):
        pltpu.make_async_remote_copy(size, size, ss, rsem.at[0, 0], device_id=(t, d), device_id_type=MESH).wait_send()

    def zrot(k):
        return (z + k) % NT

    def zback(k):
        return (z + NT - k) % NT

    loads = [
        pltpu.make_async_copy(a, b, lsem.at[2 + i])
        for i, (a, b) in enumerate([(inp_hbm, xg.at[d]), (qry_hbm, qry), (key_hbm, keyr), (tgt_hbm, tgt)])
    ]
    for cp in loads:
        cp.start()
    vcopy = pltpu.make_async_copy(v_hbm, v, lsem.at[0])
    vcopy.start()
    ocopy = pltpu.make_async_copy(o_hbm.at[:, pl.ds(d * SH, SH)], osh.at[d], lsem.at[1])
    ocopy.start()

    bar = pltpu.get_barrier_semaphore()
    greet = [(t, peer(k, -1)) for k in range(1, NT)]
    greet += [(zback(k) * 4 + il, d) for k in range(1, NT)]
    greet += [(side, peer(k, -1)) for k in range(NT)]
    greet += [(partner, d), (quad[3], d)]
    for dev in greet:
        pl.semaphore_signal(bar, inc=1, device_id=dev, device_id_type=MESH)

    loads[1].wait()
    loads[2].wait()
    row = lax.broadcasted_iota(jnp.int32, (TL, TL), 0)
    col = lax.broadcasted_iota(jnp.int32, (TL, TL), 1)
    for h in range(2):
        s = mm_nt(qry[:, h * HD:(h + 1) * HD], keyr[:, h * HD:(h + 1) * HD]) / jnp.sqrt(F32(HD))
        s = jnp.where(row >= col, s, F32(-1e30))
        s = s - jnp.max(s, axis=-1, keepdims=True)
        e = jnp.exp(s)
        probs[h] = (e / jnp.sum(e, axis=-1, keepdims=True)).astype(BF)

    pl.semaphore_wait(bar, len(greet))

    pending = []
    ZW = 4 if NT % 4 == 0 else 2
    PR = HD // ZW

    def piece_of(zz, lo=0, n=PR):
        return pl.ds(c * HD + (zz % ZW) * PR + lo, n)

    mine_p = piece_of(z)
    if ZW == 4:
        shares = [(zrot(1), zback(1), 0, PR), (zback(1), zrot(1), 0, PR)]
        shares += [(zrot(2), zback(2), 0, PR // 2), (zback(2), zrot(2), PR // 2, PR // 2)]
    else:
        shares = [(zrot(1), zback(1), 0, PR // 2), (zback(1), zrot(1), PR // 2, PR // 2)]
    for k in order:
        p = peer(k, 1)
        pending.append(
            send(o_hbm.at[mine_p, pl.ds(p * SH, SH)], osh.at[d, mine_p], ssem.at[1, k], rsem.at[1, k], (t, p))
        )
    loads[0].wait()
    direct = [k for k in order if k <= NY]
    for k in direct:
        pending.append(send(xg.at[d], xg.at[d], ssem.at[0, k], rsem.at[0, k], (t, peer(k, 1))))
    loads[3].wait()

    def mix(u):
        ub = u.astype(BF)
        return jnp.concatenate([mm(probs[h], ub[:, h * HD:(h + 1) * HD]) for h in range(2)], axis=1)

    def mix_t(u):
        ub = u.astype(BF)
        return jnp.concatenate([mm_tn(probs[h], ub[:, h * HD:(h + 1) * HD]) for h in range(2)], axis=1)

    split = spl[0]
    pos = lax.broadcasted_iota(jnp.int32, (TL, 1), 0)
    sup = jnp.where(pos < split, F32(1.0), F32(0.0))
    ns = jnp.full((TL, 1), split, jnp.int32).astype(F32)
    s_w = sup / ns
    q_w = (1.0 - sup) / (F32(TL) - ns)
    is_s = pos < split
    posr = lax.broadcasted_iota(jnp.int32, (1, TL), 1)
    q_row = jnp.where(posr < split, F32(0.0), F32(1.0)) / (F32(TL) - jnp.full((1, TL), split, jnp.int32).astype(F32))

    a0 = xg[d].astype(F32) - tgt[...].astype(F32)

    if NX > 1:
        src = peer(NY, -1)
        arrived(xg.at[src], rsem.at[0, NY])
        for k in order:
            if k < NY:
                pending.append(
                    send(xg.at[src], xg.at[src], ssem.at[0, NY + k], rsem.at[0, NY + k], (t, peer(k, 1)))
                )
    for k in order[::-1]:
        src = peer(k, -1)
        arrived(osh.at[src, mine_p], rsem.at[1, k])
        for i, (to, _, lo, n) in enumerate(shares):
            part = osh.at[src, piece_of(z, lo, n)]
            pending.append(send(part, part, fsem.at[0, i, k], fsem.at[1, i, k], (to * 4 + il, d)))
    ss = jnp.zeros((TL, 1), F32)
    for k in [0] + order[::-1]:
        src = peer(k, -1)
        if k and (NX == 1 or k != NY):
            arrived(xg.at[src], rsem.at[0, k])
        xv = xg[src].astype(F32)
        ss = ss + jnp.sum(xv * xv, axis=-1, keepdims=True)
    scale = lax.rsqrt(ss / F32(SH * NT) + F32(1e-05))
    vcopy.wait()
    u = jnp.zeros((TL, 2 * HD), F32)
    kacc = jnp.zeros((TL, TL), F32)
    for j in range(NT):
        xb = (xg[j].astype(F32) * scale).astype(BF)
        xn[j] = xb
        u = u + mm(xb, v[j * SH:(j + 1) * SH, :])
        kacc = kacc + mm_nt(xb, xb)
    kmat[...] = kacc.astype(BF)
    u = u.astype(BF).astype(F32)

    ZP, DZ, Z0 = pl.ds(0, TL), pl.ds(TL, TL), pl.ds(2 * TL, TL)

    def gather_start(part, phase):
        for k in order:
            pending.append(
                send(zc.at[d, part], zc.at[d, part], ssem.at[phase, k], rsem.at[phase, k], (t, peer(k, 1)))
            )

    zc[d, Z0, :] = mix(u).astype(BF)
    gather_start(Z0, 2)

    for k in order[::-1]:
        src = peer(k, -1)
        for i, (_, frm, lo, n) in enumerate(shares):
            arrived(osh.at[src, piece_of(frm, lo, n)], fsem.at[1, i, k])
        part = osh.at[src, pl.ds(c * HD, HD)]
        pending.append(send(part, part, fsem.at[0, 4, k], fsem.at[1, 4, k], (partner, d)))
    ocopy.wait()
    for k in order[::-1]:
        src = peer(k, -1)
        arrived(osh.at[src, pl.ds((1 - c) * HD, HD)], fsem.at[1, 4, k])

    GH = NT // 2
    RI = 2 * HD // NT
    mine_g = pl.ds(c * GH, GH)
    mine_r = pl.ds(z * RI, RI)
    rows = jnp.concatenate([osh[c * GH + g, mine_r, :] for g in range(GH)], axis=0)
    for k in order:
        p = peer(k, 1)
        gp_send[k] = mm_nt(rows, osh[p]).astype(BF)
        pending.append(send(gp_send.at[k], gp_recv.at[k], ssem.at[5, k], rsem.at[5, k], (t, p)))
    gram = mm_nt(rows, osh[d])

    NC = 4 if NT % 4 == 0 else 1
    CH = NT // NC

    def columns_start(part):
        for r in range(1, 4):
            send(
                xn.at[pl.ds(part * CH, CH), :, pl.ds(quad_il[r] * HD, HD)],
                xc.at[pl.ds(part * CH, CH), pl.ds(il * TL, TL), :],
                csem.at[0, r, part], csem.at[1, r, part], (quad[r], d),
            )

    acc = a0
    for k in [0] + order[::-1]:
        src = peer(k, -1)
        if k:
            arrived(zc.at[src, Z0], rsem.at[2, k])
        acc = acc + mm(zc[src, Z0, :], osh[src])
    err = (acc * s_w).astype(BF)
    a0b = a0.astype(BF)
    mixed = jnp.where(is_s, acc * s_w, a0).astype(BF)
    fer[1] = err
    for k in order:
        p = peer(k, 1)
        rs_send[k] = mm_nt(mixed, osh[p]).astype(BF)
        pending.append(send(rs_send.at[k], rs_recv.at[k], ssem.at[3, k], rsem.at[3, k], (t, p)))
    own = mm_nt(mixed, osh[d])
    for k in order[::-1]:
        arrived(gp_recv.at[k], rsem.at[5, k])
        gram = gram + gp_recv[k].astype(F32)
    for g in range(GH):
        gm[c * GH + g, mine_r, :] = gram[g * RI:(g + 1) * RI, :].astype(BF)
    zorder = sorted(range(1, NT), key=lambda k: -min(k, NT - k))
    for k in zorder:
        part = gm.at[mine_g, mine_r, :]
        pending.append(send(part, part, msem.at[0, k], msem.at[1, k], (zrot(k) * 4 + il, d)))
    columns_start(0)
    if NC > 1:
        columns_start(1)
    xc[:, pl.ds(il * TL, TL), :] = xn[:, :, pl.ds(il * HD, HD)]
    ea = mm_nt(err, a0b)
    ee = mm_nt(err, err)
    for k in order[::-1]:
        arrived(rs_recv.at[k], rsem.at[3, k])
        own = own + rs_recv[k].astype(F32)
    dz = jnp.where(is_s, own, F32(0.0))
    a0o = jnp.where(is_s, F32(0.0), own)
    dzb = dz.astype(BF)
    u2 = u - RATE * mm(kmat[...], mix_t(dz).astype(BF))
    z2 = mix(u2).astype(BF)
    shares = jnp.concatenate([mm_nt(dzb, z2) + ea, ee], axis=1)
    zc[d, ZP, :] = jnp.where(is_s, shares, z2.astype(F32)).astype(BF)
    gather_start(ZP, 4)
    for k in zorder:
        arrived(gm.at[mine_g, pl.ds(zback(k) * RI, RI), :], msem.at[1, k])
    pending.append(send(gm.at[mine_g], gm.at[mine_g], nsem.at[0], nsem.at[1], (partner, d)))
    arrived(gm.at[pl.ds((1 - c) * GH, GH)], nsem.at[1])

    zz = jnp.zeros((TL, TL), F32)
    tot = jnp.zeros((TL, 2 * HD), F32)
    fo = a0o
    for k in [0] + order[::-1]:
        src = peer(k, -1)
        if k:
            arrived(zc.at[src, ZP], rsem.at[4, k])
        zp = zc[src, ZP, :]
        zz = zz + mm_nt(zp, zc[src, Z0, :])
        fo = fo + mm(zp, gm[src])
        tot = tot + zp.astype(F32)
    zzb = jnp.where(is_s, F32(0.0), RATE * zz).astype(BF)
    ef = jnp.where(is_s, tot[:, :TL], F32(0.0))
    eeb = jnp.where(is_s, tot[:, TL:], F32(0.0)).astype(BF)
    fet = (-RATE * q_row * (ef - mm_nt(eeb, zzb))).astype(BF)
    fo = q_w * (fo - mm(zzb, dzb))
    dz2 = fo + mm_tn(fet, zc[d, Z0, :])
    zc[d, DZ, :] = mix(-RATE * mm(kmat[...], mix_t(dz2).astype(BF))).astype(BF)
    gather_start(DZ, 6)
    @pl.when(c == 0)
    def _():
        for part in range(2, NC):
            columns_start(part)

    acc = a0 - mm(zzb, fer[1])
    for j in range(NT):
        acc = acc + mm(zc[j, ZP, :], osh[j])
    fer[0] = (acc * q_w).astype(BF)
    acc = -mm_tn(zzb, fer[0])
    y_in = -mm_tn(zzb, fo.astype(BF))
    y_fix = mm(fet, z2)
    for k in [0] + order[::-1]:
        src = peer(k, -1)
        if k:
            arrived(zc.at[src, DZ], rsem.at[6, k])
        y_in = y_in + mm(zc[src, DZ, :], gm[src])
        acc = acc + mm(zc[src, DZ, :], osh[src])
    wall[pl.ds(il * TL, TL), :] = mix_t(dz2 + s_w * y_in + y_fix).astype(BF)
    for r in (2, 1):
        mine = wall.at[pl.ds(il * TL, TL), :]
        pending.append(send(mine, mine, wsem.at[0, r], wsem.at[1, r], (quad[r], d)))

    @pl.when(c == 1)
    def _():
        for part in range(2, NC):
            columns_start(part)

    fer[2] = (acc * s_w).astype(BF)
    errs = jnp.concatenate([fer[0], fer[1], fer[2]], axis=0)
    todo = order + [0]
    LAG = 3

    def piece(h):
        return pl.ds(h * (2 * HD // PH), 2 * HD // PH)

    def plane_start(h, rel, k):
        xt = xl + rel - 2 * rel * xl
        pending.append(
            send(
                xs_o.at[rel, k, piece(h)], xr_o.at[xl, d, piece(h)],
                hsem.at[h, rel, k], isem.at[h, xl, d], (z * 4 + xt * 2 + c, peer(k, 1)),
            )
        )

    for i in range(NT + LAG):
        if i < NT:
            j = peer(todo[i], 1)
            blk = mm_tn(zc[j], errs)
            for q in range(4):
                gob[q % 2, q // 2, j] = blk[:, q * HD:(q + 1) * HD].astype(BF)
            pending.append(
                send(gob.at[1 - c, :, j], cr_o.at[:, j], gsem.at[0, todo[i]], gsem.at[1, todo[i]], (partner, d))
            )
        if i >= LAG:
            k = todo[i - LAG]
            j = peer(k, 1)
            arrived(cr_o.at[:, j], gsem.at[1, k])
            for rel in (1, 0):
                xt = xl + rel - 2 * rel * xl
                tot = gob[c, xt, j].astype(F32) + cr_o[xt, j].astype(F32)
                if rel == 0 and k == 0:
                    xr_o[xl, d] = tot.astype(BF)
                else:
                    xs_o[rel, k] = tot.astype(BF)
                    plane_start(0, rel, k)
    for h in range(1, PH):
        for k in todo:
            for rel in (1, 0):
                if rel or k:
                    plane_start(h, rel, k)

    for part in range(NC):
        for r in range(1, 4):
            arrived(xc.at[pl.ds(part * CH, CH), pl.ds(quad_il[r] * TL, TL), :], csem.at[1, r, part])
    theirs = wall.at[pl.ds(quad_il[2] * TL, TL), :]
    arrived(theirs, wsem.at[1, 2])
    pending.append(send(theirs, theirs, wsem.at[0, 3], wsem.at[1, 3], (partner, d)))
    for r in (1, 3):
        arrived(wall.at[pl.ds(quad_il[r] * TL, TL), :], wsem.at[1, r])
    DN = NT // 2
    UP = NT - 1 - DN

    def v_block(zt):
        return mm_tn(xc[zt], wall[...])

    def ring(way, hop, total):
        to = zback(1) if way == 0 else zrot(1)
        zs_v[way, hop] = total.astype(BF)
        pending.append(
            send(
                zs_v.at[way, hop], zr_v.at[way, hop], psem.at[way, hop], qsem.at[way, hop], (to * 4 + il, d)
            )
        )

    def ring_first():
        ring(0, 0, v_block(zback(DN)))
        if UP:
            ring(1, 0, v_block(zrot(UP)))

    def ring_next(hop):
        for way, count in ((0, DN), (1, UP)):
            if hop < count:
                blk = v_block(zback(DN - hop) if way == 0 else zrot(UP - hop))
                arrived(zr_v.at[way, hop - 1], qsem.at[way, hop - 1])
                ring(way, hop, blk + zr_v[way, hop - 1].astype(F32))

    def plane_o(h, k):
        zt = zrot(k)
        for xs in range(2):

            @pl.when((xl != xs) | (d != zt))
            def _():
                arrived(xr_o.at[xs, zt, piece(h)], isem.at[h, xs, zt])

        tot = xr_o[0, zt, piece(h)].astype(F32) + xr_o[1, zt, piece(h)].astype(F32)
        if k:
            zs_o[k, piece(h)] = tot.astype(BF)
            pending.append(
                send(
                    zs_o.at[k, piece(h)], zr_o.at[k, piece(h)], tsem.at[0, h, k], tsem.at[1, h, k],
                    (zt * 4 + il, d),
                )
            )
        return tot

    ring_first()
    own_o = []
    if DN > 1:
        ring_next(1)
    for k in zorder + [0]:
        tot = plane_o(0, k)
    own_o.append(tot)
    if DN > 2:
        ring_next(2)
    for k in zorder + [0]:
        tot = plane_o(1, k)
    own_o.append(tot)
    if DN > 3:
        ring_next(3)
    own_v = v_block(z)
    for way, count in ((0, DN), (1, UP)):
        if count:
            arrived(zr_v.at[way, count - 1], qsem.at[way, count - 1])
            own_v = own_v + zr_v[way, count - 1].astype(F32)
    out_v[...] = own_v
    for h in range(PH):
        tot = own_o[h]
        for k in zorder[::-1]:
            arrived(zr_o.at[k, piece(h)], tsem.at[1, h, k])
            tot = tot + zr_o[k, piece(h)].astype(F32)
        out_o[piece(h), :] = tot

    for cp in pending:
        cp.wait_send()
    for r in range(1, 4):
        for part in range(NC):
            sent(xc.at[pl.ds(0, CH), pl.ds(0, TL), :], csem.at[0, r, part])


def finish(a_ref, b_ref, out_v, out_o):
    out_v[...] = a_ref[...]
    out_o[...] = b_ref[...]


def per_device(inputs, targets, queries, key_rows, value_weight, output_weight, splits, *, NT):
    NX = 2 if NT % 8 == 0 else 1
    NY = NT // NX
    SH = inputs.shape[1]
    vm = pltpu.VMEM
    vspec = pl.BlockSpec(memory_space=pltpu.VMEM)
    aspec = pl.BlockSpec(memory_space=pl.ANY)
    dma = pltpu.SemaphoreType.DMA
    parts = pl.pallas_call(
        functools.partial(body, NT, NX, NY),
        out_shape=(
            jax.ShapeDtypeStruct((TL, 2 * HD), F32),
            jax.ShapeDtypeStruct((2 * HD, TL), F32),
        ),
        in_specs=[aspec] * 6 + [pl.BlockSpec(memory_space=pltpu.SMEM)],
        out_specs=(vspec, vspec),
        scratch_shapes=[
            vm((SH * NT, 2 * HD), BF),
            vm((NT, TL, SH), BF),
            vm((NT, TL, SH), BF),
            vm((NT, 2 * HD, SH), BF),
            vm((NT, 3 * TL, 2 * HD), BF),
            vm((3, TL, SH), BF),
            vm((NT, TL, 2 * HD), BF),
            vm((NT, TL, 2 * HD), BF),
            vm((TL, TL), BF),
            vm((2, TL, TL), BF),
            vm((2, 2, NT, 2 * HD, HD), BF),
            vm((2, NT, 2 * HD, HD), BF),
            vm((2, NT, 2 * HD, HD), BF),
            vm((2, NT, 2 * HD, HD), BF),
            vm((NT, 2 * HD, HD), BF),
            vm((NT, 2 * HD, HD), BF),
            vm((NT, 4 * TL, HD), BF),
            vm((4 * TL, 2 * HD), BF),
            vm((2, NT // 2, TL, 2 * HD), BF),
            vm((2, NT // 2, TL, 2 * HD), BF),
            vm((NT, TL, 2 * HD), BF),
            vm((NT, TL, 2 * HD), BF),
            vm((NT, 2 * HD, 2 * HD), BF),
            vm((TL, SH), BF),
            vm((TL, 2 * HD), BF),
            vm((TL, 2 * HD), BF),
            dma((6,)),
            dma((8, NT)),
            dma((8, NT)),
            dma((2, 5, NT)),
            dma((2, NT)),
            dma((PH, 2, NT)),
            dma((PH, 2, NT)),
            dma((2, 4)),
            dma((2, 4, 4)),
            dma((2, NT)),
            dma((2, NT)),
            dma((2, NT)),
            dma((4,)),
            dma((2, PH, NT)),
        ],
        compiler_params=pltpu.CompilerParams(
            collective_id=0, has_side_effects=True, vmem_limit_bytes=60 * 1024 * 1024
        ),
        name="meta",
    )(inputs, targets, queries, key_rows, value_weight, output_weight, splits)
    return pl.pallas_call(
        finish,
        out_shape=(
            jax.ShapeDtypeStruct((TL, 2 * HD), F32),
            jax.ShapeDtypeStruct((2 * HD, TL), F32),
        ),
        in_specs=[vspec] * 2,
        out_specs=(vspec, vspec),
        name="finish",
    )(*parts)


def solution(mesh):
    return jax.shard_map(
        functools.partial(per_device, NT=mesh.shape["tensor"]),
        mesh=mesh,
        in_specs=(
            P("task", "tensor"),
            P("task", "tensor"),
            P("task", "tensor"),
            P("task", "tensor"),
            P(None, "tensor"),
            P("tensor", None),
            P("task"),
        ),
        out_specs=(P("task", "tensor"), P("tensor", "task")),
        check_vma=False,
    )
```

```python
import functools

import jax
import jax.numpy as jnp
from jax import lax
from jax.experimental import pallas as pl
from jax.experimental.pallas import tpu as pltpu
from jax.sharding import PartitionSpec as P

HD = 128
TL = 128
RATE = 0.25
PH = 2
MESH = pl.DeviceIdType.MESH
BF = jnp.bfloat16
F32 = jnp.float32


def mm(a, b):
    return lax.dot_general(a, b, (((1,), (0,)), ((), ())), preferred_element_type=F32)


def mm_nt(a, b):
    return lax.dot_general(a, b, (((1,), (1,)), ((), ())), preferred_element_type=F32)


def mm_tn(a, b):
    return lax.dot_general(a, b, (((0,), (0,)), ((), ())), preferred_element_type=F32)


def body(
    NT, NX, NY,
    inp_hbm, tgt_hbm, qry_hbm, key_hbm, v_hbm, o_hbm, spl,
    out_v, out_o,
    v, xg, xn, osh, zc, fer, rs_send, rs_recv, kmat, probs,
    gob, cr_o, xs_o, xr_o, zs_o, zr_o, xc, wall, zs_v, zr_v, gp_send, gp_recv, gm, tgt, qry, keyr,
    lsem, ssem, rsem, fsem, gsem, hsem, isem, wsem, csem, psem, qsem, msem, nsem, tsem,
):
    t = lax.axis_index("task")
    d = lax.axis_index("tensor")
    z, xl, c = t // 4, (t // 2) % 2, t % 2
    xh, y = d // NY, d % NY
    il = xl * 2 + c
    quad_il = [il, xl * 2 + 1 - c, (1 - xl) * 2 + c, (1 - xl) * 2 + 1 - c]
    quad = [z * 4 + q for q in quad_il]
    partner, side = quad[1], quad[2]
    SH = inp_hbm.shape[1]
    steps = [(a, b) for a in range(NX) for b in range(NY)]
    order = sorted(range(1, NT), key=lambda k: -(2 * steps[k][0] + min(steps[k][1], NY - steps[k][1])))

    def peer(k, sign):
        a, b = steps[k]
        return ((xh + sign * a + NX) % NX) * NY + (y + sign * b + NY) % NY

    def send(src, dst, ss, rs, dev):
        cp = pltpu.make_async_remote_copy(src, dst, ss, rs, device_id=dev, device_id_type=MESH)
        cp.start()
        return cp

    def arrived(dst, rs):
        pltpu.make_async_remote_copy(dst, dst, ssem.at[0, 0], rs, device_id=(t, d), device_id_type=MESH).wait_recv()

    def sent(size, ss):
        pltpu.make_async_remote_copy(size, size, ss, rsem.at[0, 0], device_id=(t, d), device_id_type=MESH).wait_send()

    def zrot(k):
        return (z + k) % NT

    def zback(k):
        return (z + NT - k) % NT

    loads = [
        pltpu.make_async_copy(a, b, lsem.at[2 + i])
        for i, (a, b) in enumerate([(inp_hbm, xg.at[d]), (qry_hbm, qry), (key_hbm, keyr), (tgt_hbm, tgt)])
    ]
    for cp in loads:
        cp.start()
    vcopy = pltpu.make_async_copy(v_hbm, v, lsem.at[0])
    vcopy.start()
    ocopy = pltpu.make_async_copy(o_hbm.at[:, pl.ds(d * SH, SH)], osh.at[d], lsem.at[1])
    ocopy.start()

    bar = pltpu.get_barrier_semaphore()
    greet = [(t, peer(k, -1)) for k in range(1, NT)]
    greet += [(zback(k) * 4 + il, d) for k in range(1, NT)]
    greet += [(side, peer(k, -1)) for k in range(NT)]
    greet += [(partner, d), (quad[3], d)]
    for dev in greet:
        pl.semaphore_signal(bar, inc=1, device_id=dev, device_id_type=MESH)

    loads[1].wait()
    loads[2].wait()
    row = lax.broadcasted_iota(jnp.int32, (TL, TL), 0)
    col = lax.broadcasted_iota(jnp.int32, (TL, TL), 1)
    for h in range(2):
        s = mm_nt(qry[:, h * HD:(h + 1) * HD], keyr[:, h * HD:(h + 1) * HD]) / jnp.sqrt(F32(HD))
        s = jnp.where(row >= col, s, F32(-1e30))
        s = s - jnp.max(s, axis=-1, keepdims=True)
        e = jnp.exp(s)
        probs[h] = (e / jnp.sum(e, axis=-1, keepdims=True)).astype(BF)

    pl.semaphore_wait(bar, len(greet))

    pending = []
    ZW = 4 if NT % 4 == 0 else 2
    PR = HD // ZW

    def piece_of(zz, lo=0, n=PR):
        return pl.ds(c * HD + (zz % ZW) * PR + lo, n)

    mine_p = piece_of(z)
    if ZW == 4:
        shares = [(zrot(1), zback(1), 0, PR), (zback(1), zrot(1), 0, PR)]
        shares += [(zrot(2), zback(2), 0, PR // 2), (zback(2), zrot(2), PR // 2, PR // 2)]
    else:
        shares = [(zrot(1), zback(1), 0, PR // 2), (zback(1), zrot(1), PR // 2, PR // 2)]
    for k in order:
        p = peer(k, 1)
        pending.append(
            send(o_hbm.at[mine_p, pl.ds(p * SH, SH)], osh.at[d, mine_p], ssem.at[1, k], rsem.at[1, k], (t, p))
        )
    loads[0].wait()
    direct = [k for k in order if k <= NY]
    for k in direct:
        pending.append(send(xg.at[d], xg.at[d], ssem.at[0, k], rsem.at[0, k], (t, peer(k, 1))))
    loads[3].wait()

    def mix(u):
        ub = u.astype(BF)
        return jnp.concatenate([mm(probs[h], ub[:, h * HD:(h + 1) * HD]) for h in range(2)], axis=1)

    def mix_t(u):
        ub = u.astype(BF)
        return jnp.concatenate([mm_tn(probs[h], ub[:, h * HD:(h + 1) * HD]) for h in range(2)], axis=1)

    split = spl[0]
    pos = lax.broadcasted_iota(jnp.int32, (TL, 1), 0)
    sup = jnp.where(pos < split, F32(1.0), F32(0.0))
    ns = jnp.full((TL, 1), split, jnp.int32).astype(F32)
    s_w = sup / ns
    q_w = (1.0 - sup) / (F32(TL) - ns)
    is_s = pos < split
    posr = lax.broadcasted_iota(jnp.int32, (1, TL), 1)
    q_row = jnp.where(posr < split, F32(0.0), F32(1.0)) / (F32(TL) - jnp.full((1, TL), split, jnp.int32).astype(F32))

    a0 = xg[d].astype(F32) - tgt[...].astype(F32)

    if NX > 1:
        src = peer(NY, -1)
        arrived(xg.at[src], rsem.at[0, NY])
        for k in order:
            if k < NY:
                pending.append(
                    send(xg.at[src], xg.at[src], ssem.at[0, NY + k], rsem.at[0, NY + k], (t, peer(k, 1)))
                )
    for k in order[::-1]:
        src = peer(k, -1)
        arrived(osh.at[src, mine_p], rsem.at[1, k])
        for i, (to, _, lo, n) in enumerate(shares):
            part = osh.at[src, piece_of(z, lo, n)]
            pending.append(send(part, part, fsem.at[0, i, k], fsem.at[1, i, k], (to * 4 + il, d)))
    ss = jnp.zeros((TL, 1), F32)
    for k in [0] + order[::-1]:
        src = peer(k, -1)
        if k and (NX == 1 or k != NY):
            arrived(xg.at[src], rsem.at[0, k])
        xv = xg[src].astype(F32)
        ss = ss + jnp.sum(xv * xv, axis=-1, keepdims=True)
    scale = lax.rsqrt(ss / F32(SH * NT) + F32(1e-05))
    vcopy.wait()
    u = jnp.zeros((TL, 2 * HD), F32)
    kacc = jnp.zeros((TL, TL), F32)
    for j in range(NT):
        xb = (xg[j].astype(F32) * scale).astype(BF)
        xn[j] = xb
        u = u + mm(xb, v[j * SH:(j + 1) * SH, :])
        kacc = kacc + mm_nt(xb, xb)
    kmat[...] = kacc.astype(BF)
    u = u.astype(BF).astype(F32)

    ZP, DZ, Z0 = pl.ds(0, TL), pl.ds(TL, TL), pl.ds(2 * TL, TL)

    def gather_pass(part, phase):
        if NX > 1:
            src = peer(NY, -1)
            arrived(zc.at[src, part], rsem.at[phase, NY])
            for k in order:
                if k < NY:
                    pending.append(
                        send(
                            zc.at[src, part], zc.at[src, part], ssem.at[phase, NY + k], rsem.at[phase, NY + k],
                            (t, peer(k, 1)),
                        )
                    )

    def gather_start(part, phase, ks):
        for k in ks:
            pending.append(
                send(zc.at[d, part], zc.at[d, part], ssem.at[phase, k], rsem.at[phase, k], (t, peer(k, 1)))
            )

    zc[d, Z0, :] = mix(u).astype(BF)
    gather_start(Z0, 2, order)

    for k in order[::-1]:
        src = peer(k, -1)
        for i, (_, frm, lo, n) in enumerate(shares):
            arrived(osh.at[src, piece_of(frm, lo, n)], fsem.at[1, i, k])
        part = osh.at[src, pl.ds(c * HD, HD)]
        pending.append(send(part, part, fsem.at[0, 4, k], fsem.at[1, 4, k], (partner, d)))
    ocopy.wait()
    for k in order[::-1]:
        src = peer(k, -1)
        arrived(osh.at[src, pl.ds((1 - c) * HD, HD)], fsem.at[1, 4, k])

    GH = NT // 2
    RI = 2 * HD // NT
    mine_g = pl.ds(c * GH, GH)
    mine_r = pl.ds(z * RI, RI)
    rows = jnp.concatenate([osh[c * GH + g, mine_r, :] for g in range(GH)], axis=0)
    for k in order:
        p = peer(k, 1)
        gp_send[k] = mm_nt(rows, osh[p]).astype(BF)
        pending.append(send(gp_send.at[k], gp_recv.at[k], ssem.at[5, k], rsem.at[5, k], (t, p)))
    gram = mm_nt(rows, osh[d])

    NC = 4 if NT % 4 == 0 else 1
    CH = NT // NC

    def columns_start(part):
        for r in range(1, 4):
            send(
                xn.at[pl.ds(part * CH, CH), :, pl.ds(quad_il[r] * HD, HD)],
                xc.at[pl.ds(part * CH, CH), pl.ds(il * TL, TL), :],
                csem.at[0, r, part], csem.at[1, r, part], (quad[r], d),
            )

    acc = a0
    for k in [0] + order[::-1]:
        src = peer(k, -1)
        if k:
            arrived(zc.at[src, Z0], rsem.at[2, k])
        acc = acc + mm(zc[src, Z0, :], osh[src])
    err = (acc * s_w).astype(BF)
    a0b = a0.astype(BF)
    mixed = jnp.where(is_s, acc * s_w, a0).astype(BF)
    fer[1] = err
    for k in order:
        p = peer(k, 1)
        rs_send[k] = mm_nt(mixed, osh[p]).astype(BF)
        pending.append(send(rs_send.at[k], rs_recv.at[k], ssem.at[3, k], rsem.at[3, k], (t, p)))
    own = mm_nt(mixed, osh[d])
    for k in order[::-1]:
        arrived(gp_recv.at[k], rsem.at[5, k])
        gram = gram + gp_recv[k].astype(F32)
    for g in range(GH):
        gm[c * GH + g, mine_r, :] = gram[g * RI:(g + 1) * RI, :].astype(BF)
    zorder = sorted(range(1, NT), key=lambda k: -min(k, NT - k))
    for k in zorder:
        part = gm.at[mine_g, mine_r, :]
        pending.append(send(part, part, msem.at[0, k], msem.at[1, k], (zrot(k) * 4 + il, d)))
    xc[:, pl.ds(il * TL, TL), :] = xn[:, :, pl.ds(il * HD, HD)]
    ea = mm_nt(err, a0b)
    ee = mm_nt(err, err)
    for k in order[::-1]:
        arrived(rs_recv.at[k], rsem.at[3, k])
        own = own + rs_recv[k].astype(F32)
    dz = jnp.where(is_s, own, F32(0.0))
    a0o = jnp.where(is_s, F32(0.0), own)
    dzb = dz.astype(BF)
    u2 = u - RATE * mm(kmat[...], mix_t(dz).astype(BF))
    z2 = mix(u2).astype(BF)
    shares = jnp.concatenate([mm_nt(dzb, z2) + ea, ee], axis=1)
    zc[d, ZP, :] = jnp.where(is_s, shares, z2.astype(F32)).astype(BF)
    gather_start(ZP, 4, direct)
    gather_pass(ZP, 4)
    columns_start(0)
    if NC > 1:
        columns_start(1)
    for k in zorder:
        arrived(gm.at[mine_g, pl.ds(zback(k) * RI, RI), :], msem.at[1, k])
    pending.append(send(gm.at[mine_g], gm.at[mine_g], nsem.at[0], nsem.at[1], (partner, d)))
    arrived(gm.at[pl.ds((1 - c) * GH, GH)], nsem.at[1])

    zz = jnp.zeros((TL, TL), F32)
    tot = jnp.zeros((TL, 2 * HD), F32)
    fo = a0o
    for k in [0] + order[::-1]:
        src = peer(k, -1)
        if k and (NX == 1 or k != NY):
            arrived(zc.at[src, ZP], rsem.at[4, k])
        zp = zc[src, ZP, :]
        zz = zz + mm_nt(zp, zc[src, Z0, :])
        fo = fo + mm(zp, gm[src])
        tot = tot + zp.astype(F32)
    zzb = jnp.where(is_s, F32(0.0), RATE * zz).astype(BF)
    ef = jnp.where(is_s, tot[:, :TL], F32(0.0))
    eeb = jnp.where(is_s, tot[:, TL:], F32(0.0)).astype(BF)
    fet = (-RATE * q_row * (ef - mm_nt(eeb, zzb))).astype(BF)
    fo = q_w * (fo - mm(zzb, dzb))
    dz2 = fo + mm_tn(fet, zc[d, Z0, :])
    zc[d, DZ, :] = mix(-RATE * mm(kmat[...], mix_t(dz2).astype(BF))).astype(BF)
    gather_start(DZ, 6, direct)
    for part in range(2, NC):
        columns_start(part)
    acc = a0 - mm(zzb, fer[1])
    for j in range(NT):
        acc = acc + mm(zc[j, ZP, :], osh[j])
    fer[0] = (acc * q_w).astype(BF)
    acc = -mm_tn(zzb, fer[0])
    y_in = -mm_tn(zzb, fo.astype(BF))
    y_fix = mm(fet, z2)
    gather_pass(DZ, 6)
    for k in [0] + order[::-1]:
        src = peer(k, -1)
        if k and (NX == 1 or k != NY):
            arrived(zc.at[src, DZ], rsem.at[6, k])
        y_in = y_in + mm(zc[src, DZ, :], gm[src])
        acc = acc + mm(zc[src, DZ, :], osh[src])
    wall[pl.ds(il * TL, TL), :] = mix_t(dz2 + s_w * y_in + y_fix).astype(BF)
    for r in (3, 2, 1):
        mine = wall.at[pl.ds(il * TL, TL), :]
        pending.append(send(mine, mine, wsem.at[0, r], wsem.at[1, r], (quad[r], d)))

    fer[2] = (acc * s_w).astype(BF)
    errs = jnp.concatenate([fer[0], fer[1], fer[2]], axis=0)
    todo = order + [0]
    LAG = 3

    def piece(h):
        return pl.ds(h * (2 * HD // PH), 2 * HD // PH)

    def plane_start(h, rel, k):
        xt = xl + rel - 2 * rel * xl
        pending.append(
            send(
                xs_o.at[rel, k, piece(h)], xr_o.at[xl, d, piece(h)],
                hsem.at[h, rel, k], isem.at[h, xl, d], (z * 4 + xt * 2 + c, peer(k, 1)),
            )
        )

    for i in range(NT + LAG):
        if i < NT:
            j = peer(todo[i], 1)
            blk = mm_tn(zc[j], errs)
            for q in range(4):
                gob[q % 2, q // 2, j] = blk[:, q * HD:(q + 1) * HD].astype(BF)
            pending.append(
                send(gob.at[1 - c, :, j], cr_o.at[:, j], gsem.at[0, todo[i]], gsem.at[1, todo[i]], (partner, d))
            )
        if i >= LAG:
            k = todo[i - LAG]
            j = peer(k, 1)
            arrived(cr_o.at[:, j], gsem.at[1, k])
            for rel in (1, 0):
                xt = xl + rel - 2 * rel * xl
                tot = gob[c, xt, j].astype(F32) + cr_o[xt, j].astype(F32)
                if rel == 0 and k == 0:
                    xr_o[xl, d] = tot.astype(BF)
                else:
                    xs_o[rel, k] = tot.astype(BF)
                    plane_start(0, rel, k)
    for h in range(1, PH):
        for k in todo:
            for rel in (1, 0):
                if rel or k:
                    plane_start(h, rel, k)

    for part in range(NC):
        for r in range(1, 4):
            arrived(xc.at[pl.ds(part * CH, CH), pl.ds(quad_il[r] * TL, TL), :], csem.at[1, r, part])
    for r in range(1, 4):
        arrived(wall.at[pl.ds(quad_il[r] * TL, TL), :], wsem.at[1, r])
    DN = NT // 2
    UP = NT - 1 - DN

    def v_block(zt):
        return mm_tn(xc[zt], wall[...])

    def ring(way, hop, total):
        to = zback(1) if way == 0 else zrot(1)
        zs_v[way, hop] = total.astype(BF)
        pending.append(
            send(
                zs_v.at[way, hop], zr_v.at[way, hop], psem.at[way, hop], qsem.at[way, hop], (to * 4 + il, d)
            )
        )

    def ring_first():
        ring(0, 0, v_block(zback(DN)))
        if UP:
            ring(1, 0, v_block(zrot(UP)))

    def ring_next(hop):
        for way, count in ((0, DN), (1, UP)):
            if hop < count:
                blk = v_block(zback(DN - hop) if way == 0 else zrot(UP - hop))
                arrived(zr_v.at[way, hop - 1], qsem.at[way, hop - 1])
                ring(way, hop, blk + zr_v[way, hop - 1].astype(F32))

    def plane_o(h, k):
        zt = zrot(k)
        for xs in range(2):

            @pl.when((xl != xs) | (d != zt))
            def _():
                arrived(xr_o.at[xs, zt, piece(h)], isem.at[h, xs, zt])

        tot = xr_o[0, zt, piece(h)].astype(F32) + xr_o[1, zt, piece(h)].astype(F32)
        if k:
            zs_o[k, piece(h)] = tot.astype(BF)
            pending.append(
                send(
                    zs_o.at[k, piece(h)], zr_o.at[k, piece(h)], tsem.at[0, h, k], tsem.at[1, h, k],
                    (zt * 4 + il, d),
                )
            )
        return tot

    ring_first()
    own_o = []
    if DN > 1:
        ring_next(1)
    for k in zorder + [0]:
        tot = plane_o(0, k)
    own_o.append(tot)
    if DN > 2:
        ring_next(2)
    for k in zorder + [0]:
        tot = plane_o(1, k)
    own_o.append(tot)
    if DN > 3:
        ring_next(3)
    own_v = v_block(z)
    for way, count in ((0, DN), (1, UP)):
        if count:
            arrived(zr_v.at[way, count - 1], qsem.at[way, count - 1])
            own_v = own_v + zr_v[way, count - 1].astype(F32)
    out_v[...] = own_v
    for h in range(PH):
        tot = own_o[h]
        for k in zorder[::-1]:
            arrived(zr_o.at[k, piece(h)], tsem.at[1, h, k])
            tot = tot + zr_o[k, piece(h)].astype(F32)
        out_o[piece(h), :] = tot

    for cp in pending:
        cp.wait_send()
    for r in range(1, 4):
        for part in range(NC):
            sent(xc.at[pl.ds(0, CH), pl.ds(0, TL), :], csem.at[0, r, part])


def per_device(inputs, targets, queries, key_rows, value_weight, output_weight, splits, *, NT):
    NX = 2 if NT % 8 == 0 else 1
    NY = NT // NX
    SH = inputs.shape[1]
    vm = pltpu.VMEM
    vspec = pl.BlockSpec(memory_space=pltpu.VMEM)
    aspec = pl.BlockSpec(memory_space=pl.ANY)
    dma = pltpu.SemaphoreType.DMA
    parts = pl.pallas_call(
        functools.partial(body, NT, NX, NY),
        out_shape=(pltpu.VMEM((TL, 2 * HD), F32), pltpu.VMEM((2 * HD, TL), F32)),
        in_specs=[aspec] * 6 + [pl.BlockSpec(memory_space=pltpu.SMEM)],
        out_specs=(vspec, vspec),
        scratch_shapes=[
            vm((SH * NT, 2 * HD), BF),
            vm((NT, TL, SH), BF),
            vm((NT, TL, SH), BF),
            vm((NT, 2 * HD, SH), BF),
            vm((NT, 3 * TL, 2 * HD), BF),
            vm((3, TL, SH), BF),
            vm((NT, TL, 2 * HD), BF),
            vm((NT, TL, 2 * HD), BF),
            vm((TL, TL), BF),
            vm((2, TL, TL), BF),
            vm((2, 2, NT, 2 * HD, HD), BF),
            vm((2, NT, 2 * HD, HD), BF),
            vm((2, NT, 2 * HD, HD), BF),
            vm((2, NT, 2 * HD, HD), BF),
            vm((NT, 2 * HD, HD), BF),
            vm((NT, 2 * HD, HD), BF),
            vm((NT, 4 * TL, HD), BF),
            vm((4 * TL, 2 * HD), BF),
            vm((2, NT // 2, TL, 2 * HD), BF),
            vm((2, NT // 2, TL, 2 * HD), BF),
            vm((NT, TL, 2 * HD), BF),
            vm((NT, TL, 2 * HD), BF),
            vm((NT, 2 * HD, 2 * HD), BF),
            vm((TL, SH), BF),
            vm((TL, 2 * HD), BF),
            vm((TL, 2 * HD), BF),
            dma((6,)),
            dma((8, NT)),
            dma((8, NT)),
            dma((2, 5, NT)),
            dma((2, NT)),
            dma((PH, 2, NT)),
            dma((PH, 2, NT)),
            dma((2, 4)),
            dma((2, 4, 4)),
            dma((2, NT)),
            dma((2, NT)),
            dma((2, NT)),
            dma((4,)),
            dma((2, PH, NT)),
        ],
        compiler_params=pltpu.CompilerParams(
            collective_id=0, has_side_effects=True, vmem_limit_bytes=60 * 1024 * 1024
        ),
        name="meta",
    )(inputs, targets, queries, key_rows, value_weight, output_weight, splits)
    return parts


def solution(mesh):
    return jax.shard_map(
        functools.partial(per_device, NT=mesh.shape["tensor"]),
        mesh=mesh,
        in_specs=(
            P("task", "tensor"),
            P("task", "tensor"),
            P("task", "tensor"),
            P("task", "tensor"),
            P(None, "tensor"),
            P("tensor", None),
            P("task"),
        ),
        out_specs=(P("task", "tensor"), P("tensor", "task")),
        check_vma=False,
    )
```

```python
import functools

import jax
import jax.numpy as jnp
from jax import lax
from jax.experimental import pallas as pl
from jax.experimental.pallas import tpu as pltpu
from jax.sharding import PartitionSpec as P

HD = 128
TL = 128
RATE = 0.25
PH = 2
MESH = pl.DeviceIdType.MESH
BF = jnp.bfloat16
F32 = jnp.float32


def mm(a, b):
    return lax.dot_general(a, b, (((1,), (0,)), ((), ())), preferred_element_type=F32)


def mm_nt(a, b):
    return lax.dot_general(a, b, (((1,), (1,)), ((), ())), preferred_element_type=F32)


def mm_tn(a, b):
    return lax.dot_general(a, b, (((0,), (0,)), ((), ())), preferred_element_type=F32)


def body(
    NT, NX, NY,
    inp_hbm, tgt_hbm, qry_hbm, key_hbm, v_hbm, o_hbm, spl,
    out_v, out_o,
    v, xg, xn, osh, zc, fer, rs_send, rs_recv, kmat, probs,
    gob, cr_o, xs_o, xr_o, zs_o, zr_o, xc, wall, zs_v, zr_v, gp_send, gp_recv, gm, tgt, qry, keyr,
    lsem, ssem, rsem, fsem, gsem, hsem, isem, wsem, csem, psem, qsem, msem, nsem, tsem,
):
    t = lax.axis_index("task")
    d = lax.axis_index("tensor")
    z, xl, c = t // 4, (t // 2) % 2, t % 2
    xh, y = d // NY, d % NY
    il = xl * 2 + c
    quad_il = [il, xl * 2 + 1 - c, (1 - xl) * 2 + c, (1 - xl) * 2 + 1 - c]
    quad = [z * 4 + q for q in quad_il]
    partner, side = quad[1], quad[2]
    SH = inp_hbm.shape[1]
    steps = [(a, b) for a in range(NX) for b in range(NY)]
    order = sorted(range(1, NT), key=lambda k: -(2 * steps[k][0] + min(steps[k][1], NY - steps[k][1])))

    def peer(k, sign):
        a, b = steps[k]
        return ((xh + sign * a + NX) % NX) * NY + (y + sign * b + NY) % NY

    def send(src, dst, ss, rs, dev):
        cp = pltpu.make_async_remote_copy(src, dst, ss, rs, device_id=dev, device_id_type=MESH)
        cp.start()
        return cp

    def arrived(dst, rs):
        pltpu.make_async_remote_copy(dst, dst, ssem.at[0, 0], rs, device_id=(t, d), device_id_type=MESH).wait_recv()

    def sent(size, ss):
        pltpu.make_async_remote_copy(size, size, ss, rsem.at[0, 0], device_id=(t, d), device_id_type=MESH).wait_send()

    def zrot(k):
        return (z + k) % NT

    def zback(k):
        return (z + NT - k) % NT

    loads = [
        pltpu.make_async_copy(a, b, lsem.at[2 + i])
        for i, (a, b) in enumerate([(inp_hbm, xg.at[d]), (qry_hbm, qry), (key_hbm, keyr), (tgt_hbm, tgt)])
    ]
    for cp in loads:
        cp.start()
    vcopy = pltpu.make_async_copy(v_hbm, v, lsem.at[0])
    vcopy.start()
    ocopy = pltpu.make_async_copy(o_hbm.at[:, pl.ds(d * SH, SH)], osh.at[d], lsem.at[1])
    ocopy.start()

    bar = pltpu.get_barrier_semaphore()
    greet = [(t, peer(k, -1)) for k in range(1, NT)]
    greet += [(zback(k) * 4 + il, d) for k in range(1, NT)]
    greet += [(side, peer(k, -1)) for k in range(NT)]
    greet += [(partner, d), (quad[3], d)]
    for dev in greet:
        pl.semaphore_signal(bar, inc=1, device_id=dev, device_id_type=MESH)

    loads[1].wait()
    loads[2].wait()
    row = lax.broadcasted_iota(jnp.int32, (TL, TL), 0)
    col = lax.broadcasted_iota(jnp.int32, (TL, TL), 1)
    for h in range(2):
        s = mm_nt(qry[:, h * HD:(h + 1) * HD], keyr[:, h * HD:(h + 1) * HD]) / jnp.sqrt(F32(HD))
        s = jnp.where(row >= col, s, F32(-1e30))
        s = s - jnp.max(s, axis=-1, keepdims=True)
        e = jnp.exp(s)
        probs[h] = (e / jnp.sum(e, axis=-1, keepdims=True)).astype(BF)

    pl.semaphore_wait(bar, len(greet))

    pending = []
    ZW = 4 if NT % 4 == 0 else 2
    PR = HD // ZW

    def piece_of(zz, lo=0, n=PR):
        return pl.ds(c * HD + (zz % ZW) * PR + lo, n)

    mine_p = piece_of(z)
    if ZW == 4:
        shares = [(zrot(1), zback(1), 0, PR), (zback(1), zrot(1), 0, PR)]
        shares += [(zrot(2), zback(2), 0, PR // 2), (zback(2), zrot(2), PR // 2, PR // 2)]
    else:
        shares = [(zrot(1), zback(1), 0, PR // 2), (zback(1), zrot(1), PR // 2, PR // 2)]
    for k in order:
        p = peer(k, 1)
        pending.append(
            send(o_hbm.at[mine_p, pl.ds(p * SH, SH)], osh.at[d, mine_p], ssem.at[1, k], rsem.at[1, k], (t, p))
        )
    loads[0].wait()
    direct = [k for k in order if k <= NY]
    for k in direct:
        pending.append(send(xg.at[d], xg.at[d], ssem.at[0, k], rsem.at[0, k], (t, peer(k, 1))))
    loads[3].wait()

    def mix(u):
        ub = u.astype(BF)
        return jnp.concatenate([mm(probs[h], ub[:, h * HD:(h + 1) * HD]) for h in range(2)], axis=1)

    def mix_t(u):
        ub = u.astype(BF)
        return jnp.concatenate([mm_tn(probs[h], ub[:, h * HD:(h + 1) * HD]) for h in range(2)], axis=1)

    split = spl[0]
    pos = lax.broadcasted_iota(jnp.int32, (TL, 1), 0)
    sup = jnp.where(pos < split, F32(1.0), F32(0.0))
    ns = jnp.full((TL, 1), split, jnp.int32).astype(F32)
    s_w = sup / ns
    q_w = (1.0 - sup) / (F32(TL) - ns)
    is_s = pos < split
    posr = lax.broadcasted_iota(jnp.int32, (1, TL), 1)
    q_row = jnp.where(posr < split, F32(0.0), F32(1.0)) / (F32(TL) - jnp.full((1, TL), split, jnp.int32).astype(F32))

    a0 = xg[d].astype(F32) - tgt[...].astype(F32)

    if NX > 1:
        src = peer(NY, -1)
        arrived(xg.at[src], rsem.at[0, NY])
        for k in order:
            if k < NY:
                pending.append(
                    send(xg.at[src], xg.at[src], ssem.at[0, NY + k], rsem.at[0, NY + k], (t, peer(k, 1)))
                )
    for k in order[::-1]:
        src = peer(k, -1)
        arrived(osh.at[src, mine_p], rsem.at[1, k])
        for i, (to, _, lo, n) in enumerate(shares):
            part = osh.at[src, piece_of(z, lo, n)]
            pending.append(send(part, part, fsem.at[0, i, k], fsem.at[1, i, k], (to * 4 + il, d)))
    ss = jnp.zeros((TL, 1), F32)
    for k in [0] + order[::-1]:
        src = peer(k, -1)
        if k and (NX == 1 or k != NY):
            arrived(xg.at[src], rsem.at[0, k])
        xv = xg[src].astype(F32)
        ss = ss + jnp.sum(xv * xv, axis=-1, keepdims=True)
    scale = lax.rsqrt(ss / F32(SH * NT) + F32(1e-05))
    vcopy.wait()
    u = jnp.zeros((TL, 2 * HD), F32)
    kacc = jnp.zeros((TL, TL), F32)
    for j in range(NT):
        xb = (xg[j].astype(F32) * scale).astype(BF)
        xn[j] = xb
        u = u + mm(xb, v[j * SH:(j + 1) * SH, :])
        kacc = kacc + mm_nt(xb, xb)
    kmat[...] = kacc.astype(BF)
    u = u.astype(BF).astype(F32)

    ZP, DZ, Z0 = pl.ds(0, TL), pl.ds(TL, TL), pl.ds(2 * TL, TL)

    def gather_pass(part, phase):
        if NX > 1:
            src = peer(NY, -1)
            arrived(zc.at[src, part], rsem.at[phase, NY])
            for k in order:
                if k < NY:
                    pending.append(
                        send(
                            zc.at[src, part], zc.at[src, part], ssem.at[phase, NY + k], rsem.at[phase, NY + k],
                            (t, peer(k, 1)),
                        )
                    )

    def gather_start(part, phase, ks):
        for k in ks:
            pending.append(
                send(zc.at[d, part], zc.at[d, part], ssem.at[phase, k], rsem.at[phase, k], (t, peer(k, 1)))
            )

    zc[d, Z0, :] = mix(u).astype(BF)
    gather_start(Z0, 2, order)

    for k in order[::-1]:
        src = peer(k, -1)
        for i, (_, frm, lo, n) in enumerate(shares):
            arrived(osh.at[src, piece_of(frm, lo, n)], fsem.at[1, i, k])
        part = osh.at[src, pl.ds(c * HD, HD)]
        pending.append(send(part, part, fsem.at[0, 4, k], fsem.at[1, 4, k], (partner, d)))
    ocopy.wait()
    for k in order[::-1]:
        src = peer(k, -1)
        arrived(osh.at[src, pl.ds((1 - c) * HD, HD)], fsem.at[1, 4, k])

    GH = NT // 2
    RI = 2 * HD // NT
    mine_g = pl.ds(c * GH, GH)
    mine_r = pl.ds(z * RI, RI)
    rows = jnp.concatenate([osh[c * GH + g, mine_r, :] for g in range(GH)], axis=0)
    for k in order:
        p = peer(k, 1)
        gp_send[k] = mm_nt(rows, osh[p]).astype(BF)
        pending.append(send(gp_send.at[k], gp_recv.at[k], ssem.at[5, k], rsem.at[5, k], (t, p)))
    gram = mm_nt(rows, osh[d])

    NC = 4 if NT % 4 == 0 else 1
    CH = NT // NC

    def columns_start(part):
        for r in range(1, 4):
            send(
                xn.at[pl.ds(part * CH, CH), :, pl.ds(quad_il[r] * HD, HD)],
                xc.at[pl.ds(part * CH, CH), pl.ds(il * TL, TL), :],
                csem.at[0, r, part], csem.at[1, r, part], (quad[r], d),
            )

    acc = a0
    for k in [0] + order[::-1]:
        src = peer(k, -1)
        if k:
            arrived(zc.at[src, Z0], rsem.at[2, k])
        acc = acc + mm(zc[src, Z0, :], osh[src])
    err = (acc * s_w).astype(BF)
    a0b = a0.astype(BF)
    mixed = jnp.where(is_s, acc * s_w, a0).astype(BF)
    fer[1] = err
    for k in order:
        p = peer(k, 1)
        rs_send[k] = mm_nt(mixed, osh[p]).astype(BF)
        pending.append(send(rs_send.at[k], rs_recv.at[k], ssem.at[3, k], rsem.at[3, k], (t, p)))
    own = mm_nt(mixed, osh[d])
    for k in order[::-1]:
        arrived(gp_recv.at[k], rsem.at[5, k])
        gram = gram + gp_recv[k].astype(F32)
    for g in range(GH):
        gm[c * GH + g, mine_r, :] = gram[g * RI:(g + 1) * RI, :].astype(BF)
    zorder = sorted(range(1, NT), key=lambda k: -min(k, NT - k))
    for k in zorder:
        part = gm.at[mine_g, mine_r, :]
        pending.append(send(part, part, msem.at[0, k], msem.at[1, k], (zrot(k) * 4 + il, d)))
    xc[:, pl.ds(il * TL, TL), :] = xn[:, :, pl.ds(il * HD, HD)]
    ea = mm_nt(err, a0b)
    ee = mm_nt(err, err)
    for k in order[::-1]:
        arrived(rs_recv.at[k], rsem.at[3, k])
        own = own + rs_recv[k].astype(F32)
    dz = jnp.where(is_s, own, F32(0.0))
    a0o = jnp.where(is_s, F32(0.0), own)
    dzb = dz.astype(BF)
    u2 = u - RATE * mm(kmat[...], mix_t(dz).astype(BF))
    z2 = mix(u2).astype(BF)
    shares = jnp.concatenate([mm_nt(dzb, z2) + ea, ee], axis=1)
    zc[d, ZP, :] = jnp.where(is_s, shares, z2.astype(F32)).astype(BF)
    gather_start(ZP, 4, direct)
    gather_pass(ZP, 4)
    columns_start(0)
    if NC > 1:
        columns_start(1)
    for k in zorder:
        arrived(gm.at[mine_g, pl.ds(zback(k) * RI, RI), :], msem.at[1, k])
    pending.append(send(gm.at[mine_g], gm.at[mine_g], nsem.at[0], nsem.at[1], (partner, d)))
    arrived(gm.at[pl.ds((1 - c) * GH, GH)], nsem.at[1])

    zz = jnp.zeros((TL, TL), F32)
    tot = jnp.zeros((TL, 2 * HD), F32)
    fo = a0o
    for k in [0] + order[::-1]:
        src = peer(k, -1)
        if k and (NX == 1 or k != NY):
            arrived(zc.at[src, ZP], rsem.at[4, k])
        zp = zc[src, ZP, :]
        zz = zz + mm_nt(zp, zc[src, Z0, :])
        fo = fo + mm(zp, gm[src])
        tot = tot + zp.astype(F32)
    zzb = jnp.where(is_s, F32(0.0), RATE * zz).astype(BF)
    ef = jnp.where(is_s, tot[:, :TL], F32(0.0))
    eeb = jnp.where(is_s, tot[:, TL:], F32(0.0)).astype(BF)
    fet = (-RATE * q_row * (ef - mm_nt(eeb, zzb))).astype(BF)
    fo = q_w * (fo - mm(zzb, dzb))
    dz2 = fo + mm_tn(fet, zc[d, Z0, :])
    zc[d, DZ, :] = mix(-RATE * mm(kmat[...], mix_t(dz2).astype(BF))).astype(BF)
    gather_start(DZ, 6, direct)
    for part in range(2, NC):
        columns_start(part)
    acc = a0 - mm(zzb, fer[1])
    for j in range(NT):
        acc = acc + mm(zc[j, ZP, :], osh[j])
    fer[0] = (acc * q_w).astype(BF)
    acc = -mm_tn(zzb, fer[0])
    y_in = -mm_tn(zzb, fo.astype(BF))
    y_fix = mm(fet, z2)
    gather_pass(DZ, 6)
    for k in [0] + order[::-1]:
        src = peer(k, -1)
        if k and (NX == 1 or k != NY):
            arrived(zc.at[src, DZ], rsem.at[6, k])
        y_in = y_in + mm(zc[src, DZ, :], gm[src])
        acc = acc + mm(zc[src, DZ, :], osh[src])
    wall[pl.ds(il * TL, TL), :] = mix_t(dz2 + s_w * y_in + y_fix).astype(BF)
    for r in (3, 2, 1):
        mine = wall.at[pl.ds(il * TL, TL), :]
        pending.append(send(mine, mine, wsem.at[0, r], wsem.at[1, r], (quad[r], d)))

    fer[2] = (acc * s_w).astype(BF)
    errs = jnp.concatenate([fer[0], fer[1], fer[2]], axis=0)
    todo = order + [0]
    LAG = 4

    def piece(h):
        return pl.ds(h * (2 * HD // PH), 2 * HD // PH)

    def plane_start(h, rel, k):
        xt = xl + rel - 2 * rel * xl
        pending.append(
            send(
                xs_o.at[rel, k, piece(h)], xr_o.at[xl, d, piece(h)],
                hsem.at[h, rel, k], isem.at[h, xl, d], (z * 4 + xt * 2 + c, peer(k, 1)),
            )
        )

    for i in range(NT + LAG):
        if i < NT:
            j = peer(todo[i], 1)
            blk = mm_tn(zc[j], errs)
            for q in range(4):
                gob[q % 2, q // 2, j] = blk[:, q * HD:(q + 1) * HD].astype(BF)
            pending.append(
                send(gob.at[1 - c, :, j], cr_o.at[:, j], gsem.at[0, todo[i]], gsem.at[1, todo[i]], (partner, d))
            )
        if i >= LAG:
            k = todo[i - LAG]
            j = peer(k, 1)
            arrived(cr_o.at[:, j], gsem.at[1, k])
            for rel in (1, 0):
                xt = xl + rel - 2 * rel * xl
                tot = gob[c, xt, j].astype(F32) + cr_o[xt, j].astype(F32)
                if rel == 0 and k == 0:
                    xr_o[xl, d] = tot.astype(BF)
                else:
                    xs_o[rel, k] = tot.astype(BF)
                    plane_start(0, rel, k)
    for h in range(1, PH):
        for k in todo:
            for rel in (1, 0):
                if rel or k:
                    plane_start(h, rel, k)

    for part in range(NC):
        for r in range(1, 4):
            arrived(xc.at[pl.ds(part * CH, CH), pl.ds(quad_il[r] * TL, TL), :], csem.at[1, r, part])
    for r in range(1, 4):
        arrived(wall.at[pl.ds(quad_il[r] * TL, TL), :], wsem.at[1, r])
    DN = NT // 2
    UP = NT - 1 - DN

    def v_block(zt):
        return mm_tn(xc[zt], wall[...])

    def ring(way, hop, total):
        to = zback(1) if way == 0 else zrot(1)
        zs_v[way, hop] = total.astype(BF)
        pending.append(
            send(
                zs_v.at[way, hop], zr_v.at[way, hop], psem.at[way, hop], qsem.at[way, hop], (to * 4 + il, d)
            )
        )

    def ring_first():
        ring(0, 0, v_block(zback(DN)))
        if UP:
            ring(1, 0, v_block(zrot(UP)))

    def ring_next(hop):
        for way, count in ((0, DN), (1, UP)):
            if hop < count:
                blk = v_block(zback(DN - hop) if way == 0 else zrot(UP - hop))
                arrived(zr_v.at[way, hop - 1], qsem.at[way, hop - 1])
                ring(way, hop, blk + zr_v[way, hop - 1].astype(F32))

    def plane_o(h, k):
        zt = zrot(k)
        for xs in range(2):

            @pl.when((xl != xs) | (d != zt))
            def _():
                arrived(xr_o.at[xs, zt, piece(h)], isem.at[h, xs, zt])

        tot = xr_o[0, zt, piece(h)].astype(F32) + xr_o[1, zt, piece(h)].astype(F32)
        if k:
            zs_o[k, piece(h)] = tot.astype(BF)
            pending.append(
                send(
                    zs_o.at[k, piece(h)], zr_o.at[k, piece(h)], tsem.at[0, h, k], tsem.at[1, h, k],
                    (zt * 4 + il, d),
                )
            )
        return tot

    ring_first()
    own_o = []
    if DN > 1:
        ring_next(1)
    if DN > 2:
        ring_next(2)
    for k in zorder + [0]:
        tot = plane_o(0, k)
    own_o.append(tot)
    for k in zorder + [0]:
        tot = plane_o(1, k)
    own_o.append(tot)
    if DN > 3:
        ring_next(3)
    own_v = v_block(z)
    for way, count in ((0, DN), (1, UP)):
        if count:
            arrived(zr_v.at[way, count - 1], qsem.at[way, count - 1])
            own_v = own_v + zr_v[way, count - 1].astype(F32)
    out_v[...] = own_v
    for h in range(PH):
        tot = own_o[h]
        for k in zorder[::-1]:
            arrived(zr_o.at[k, piece(h)], tsem.at[1, h, k])
            tot = tot + zr_o[k, piece(h)].astype(F32)
        out_o[piece(h), :] = tot

    for cp in pending:
        cp.wait_send()
    for r in range(1, 4):
        for part in range(NC):
            sent(xc.at[pl.ds(0, CH), pl.ds(0, TL), :], csem.at[0, r, part])


def per_device(inputs, targets, queries, key_rows, value_weight, output_weight, splits, *, NT):
    NX = 2 if NT % 8 == 0 else 1
    NY = NT // NX
    SH = inputs.shape[1]
    vm = pltpu.VMEM
    vspec = pl.BlockSpec(memory_space=pltpu.VMEM)
    aspec = pl.BlockSpec(memory_space=pl.ANY)
    dma = pltpu.SemaphoreType.DMA
    parts = pl.pallas_call(
        functools.partial(body, NT, NX, NY),
        out_shape=(pltpu.VMEM((TL, 2 * HD), F32), pltpu.VMEM((2 * HD, TL), F32)),
        in_specs=[aspec] * 6 + [pl.BlockSpec(memory_space=pltpu.SMEM)],
        out_specs=(vspec, vspec),
        scratch_shapes=[
            vm((SH * NT, 2 * HD), BF),
            vm((NT, TL, SH), BF),
            vm((NT, TL, SH), BF),
            vm((NT, 2 * HD, SH), BF),
            vm((NT, 3 * TL, 2 * HD), BF),
            vm((3, TL, SH), BF),
            vm((NT, TL, 2 * HD), BF),
            vm((NT, TL, 2 * HD), BF),
            vm((TL, TL), BF),
            vm((2, TL, TL), BF),
            vm((2, 2, NT, 2 * HD, HD), BF),
            vm((2, NT, 2 * HD, HD), BF),
            vm((2, NT, 2 * HD, HD), BF),
            vm((2, NT, 2 * HD, HD), BF),
            vm((NT, 2 * HD, HD), BF),
            vm((NT, 2 * HD, HD), BF),
            vm((NT, 4 * TL, HD), BF),
            vm((4 * TL, 2 * HD), BF),
            vm((2, NT // 2, TL, 2 * HD), BF),
            vm((2, NT // 2, TL, 2 * HD), BF),
            vm((NT, TL, 2 * HD), BF),
            vm((NT, TL, 2 * HD), BF),
            vm((NT, 2 * HD, 2 * HD), BF),
            vm((TL, SH), BF),
            vm((TL, 2 * HD), BF),
            vm((TL, 2 * HD), BF),
            dma((6,)),
            dma((8, NT)),
            dma((8, NT)),
            dma((2, 5, NT)),
            dma((2, NT)),
            dma((PH, 2, NT)),
            dma((PH, 2, NT)),
            dma((2, 4)),
            dma((2, 4, 4)),
            dma((2, NT)),
            dma((2, NT)),
            dma((2, NT)),
            dma((4,)),
            dma((2, PH, NT)),
        ],
        compiler_params=pltpu.CompilerParams(
            collective_id=0, has_side_effects=True, vmem_limit_bytes=60 * 1024 * 1024
        ),
        name="meta",
    )(inputs, targets, queries, key_rows, value_weight, output_weight, splits)
    return parts


def solution(mesh):
    return jax.shard_map(
        functools.partial(per_device, NT=mesh.shape["tensor"]),
        mesh=mesh,
        in_specs=(
            P("task", "tensor"),
            P("task", "tensor"),
            P("task", "tensor"),
            P("task", "tensor"),
            P(None, "tensor"),
            P("tensor", None),
            P("task"),
        ),
        out_specs=(P("task", "tensor"), P("tensor", "task")),
        check_vma=False,
    )
```

```python
import functools

import jax
import jax.numpy as jnp
from jax import lax
from jax.experimental import pallas as pl
from jax.experimental.pallas import tpu as pltpu
from jax.sharding import PartitionSpec as P

HD = 128
TL = 128
RATE = 0.25
PH = 2
MESH = pl.DeviceIdType.MESH
BF = jnp.bfloat16
F32 = jnp.float32


def mm(a, b):
    return lax.dot_general(a, b, (((1,), (0,)), ((), ())), preferred_element_type=F32)


def mm_nt(a, b):
    return lax.dot_general(a, b, (((1,), (1,)), ((), ())), preferred_element_type=F32)


def mm_tn(a, b):
    return lax.dot_general(a, b, (((0,), (0,)), ((), ())), preferred_element_type=F32)


def body(
    NT, NX, NY,
    inp_hbm, tgt_hbm, qry_hbm, key_hbm, v_hbm, o_hbm, spl,
    out_v, out_o,
    v, xg, xn, osh, zc, fer, rs_send, rs_recv, kmat, probs,
    gob, cr_o, xs_o, xr_o, zs_o, zr_o, xc, wall, zs_v, zr_v, gp_send, gp_recv, gm, tgt, qry, keyr,
    lsem, ssem, rsem, fsem, gsem, hsem, isem, wsem, csem, psem, qsem, msem, nsem, tsem,
):
    t = lax.axis_index("task")
    d = lax.axis_index("tensor")
    z, xl, c = t // 4, (t // 2) % 2, t % 2
    xh, y = d // NY, d % NY
    il = xl * 2 + c
    quad_il = [il, xl * 2 + 1 - c, (1 - xl) * 2 + c, (1 - xl) * 2 + 1 - c]
    quad = [z * 4 + q for q in quad_il]
    partner, side = quad[1], quad[2]
    SH = inp_hbm.shape[1]
    steps = [(a, b) for a in range(NX) for b in range(NY)]
    order = sorted(range(1, NT), key=lambda k: -(2 * steps[k][0] + min(steps[k][1], NY - steps[k][1])))

    def peer(k, sign):
        a, b = steps[k]
        return ((xh + sign * a + NX) % NX) * NY + (y + sign * b + NY) % NY

    def send(src, dst, ss, rs, dev):
        cp = pltpu.make_async_remote_copy(src, dst, ss, rs, device_id=dev, device_id_type=MESH)
        cp.start()
        return cp

    def arrived(dst, rs):
        pltpu.make_async_remote_copy(dst, dst, ssem.at[0, 0], rs, device_id=(t, d), device_id_type=MESH).wait_recv()

    def sent(size, ss):
        pltpu.make_async_remote_copy(size, size, ss, rsem.at[0, 0], device_id=(t, d), device_id_type=MESH).wait_send()

    def zrot(k):
        return (z + k) % NT

    def zback(k):
        return (z + NT - k) % NT

    loads = [
        pltpu.make_async_copy(a, b, lsem.at[2 + i])
        for i, (a, b) in enumerate([(inp_hbm, xg.at[d]), (qry_hbm, qry), (key_hbm, keyr), (tgt_hbm, tgt)])
    ]
    for cp in loads:
        cp.start()
    vcopy = pltpu.make_async_copy(v_hbm, v, lsem.at[0])
    vcopy.start()
    ocopy = pltpu.make_async_copy(o_hbm.at[:, pl.ds(d * SH, SH)], osh.at[d], lsem.at[1])
    ocopy.start()

    bar = pltpu.get_barrier_semaphore()
    greet = [(t, peer(k, -1)) for k in range(1, NT)]
    greet += [(zback(k) * 4 + il, d) for k in range(1, NT)]
    greet += [(side, peer(k, -1)) for k in range(NT)]
    greet += [(partner, d), (quad[3], d)]
    for dev in greet:
        pl.semaphore_signal(bar, inc=1, device_id=dev, device_id_type=MESH)

    loads[1].wait()
    loads[2].wait()
    row = lax.broadcasted_iota(jnp.int32, (TL, TL), 0)
    col = lax.broadcasted_iota(jnp.int32, (TL, TL), 1)
    for h in range(2):
        s = mm_nt(qry[:, h * HD:(h + 1) * HD], keyr[:, h * HD:(h + 1) * HD]) / jnp.sqrt(F32(HD))
        s = jnp.where(row >= col, s, F32(-1e30))
        s = s - jnp.max(s, axis=-1, keepdims=True)
        e = jnp.exp(s)
        probs[h] = (e / jnp.sum(e, axis=-1, keepdims=True)).astype(BF)

    pl.semaphore_wait(bar, len(greet))

    pending = []
    ZW = 4 if NT % 4 == 0 else 2
    PR = HD // ZW

    def piece_of(zz, lo=0, n=PR):
        return pl.ds(c * HD + (zz % ZW) * PR + lo, n)

    mine_p = piece_of(z)
    if ZW == 4:
        shares = [(zrot(1), zback(1), 0, PR), (zback(1), zrot(1), 0, PR)]
        shares += [(zrot(2), zback(2), 0, PR // 2), (zback(2), zrot(2), PR // 2, PR // 2)]
    else:
        shares = [(zrot(1), zback(1), 0, PR // 2), (zback(1), zrot(1), PR // 2, PR // 2)]
    for k in order:
        p = peer(k, 1)
        pending.append(
            send(o_hbm.at[mine_p, pl.ds(p * SH, SH)], osh.at[d, mine_p], ssem.at[1, k], rsem.at[1, k], (t, p))
        )
    loads[0].wait()
    direct = [k for k in order if k <= NY]
    for k in direct:
        pending.append(send(xg.at[d], xg.at[d], ssem.at[0, k], rsem.at[0, k], (t, peer(k, 1))))
    loads[3].wait()

    def mix(u):
        ub = u.astype(BF)
        return jnp.concatenate([mm(probs[h], ub[:, h * HD:(h + 1) * HD]) for h in range(2)], axis=1)

    def mix_t(u):
        ub = u.astype(BF)
        return jnp.concatenate([mm_tn(probs[h], ub[:, h * HD:(h + 1) * HD]) for h in range(2)], axis=1)

    split = spl[0]
    pos = lax.broadcasted_iota(jnp.int32, (TL, 1), 0)
    sup = jnp.where(pos < split, F32(1.0), F32(0.0))
    ns = jnp.full((TL, 1), split, jnp.int32).astype(F32)
    s_w = sup / ns
    q_w = (1.0 - sup) / (F32(TL) - ns)
    is_s = pos < split
    posr = lax.broadcasted_iota(jnp.int32, (1, TL), 1)
    q_row = jnp.where(posr < split, F32(0.0), F32(1.0)) / (F32(TL) - jnp.full((1, TL), split, jnp.int32).astype(F32))

    a0 = xg[d].astype(F32) - tgt[...].astype(F32)

    if NX > 1:
        src = peer(NY, -1)
        arrived(xg.at[src], rsem.at[0, NY])
        for k in order:
            if k < NY:
                pending.append(
                    send(xg.at[src], xg.at[src], ssem.at[0, NY + k], rsem.at[0, NY + k], (t, peer(k, 1)))
                )
    for k in order[::-1]:
        src = peer(k, -1)
        arrived(osh.at[src, mine_p], rsem.at[1, k])
        for i, (to, _, lo, n) in enumerate(shares):
            part = osh.at[src, piece_of(z, lo, n)]
            pending.append(send(part, part, fsem.at[0, i, k], fsem.at[1, i, k], (to * 4 + il, d)))
    ss = jnp.zeros((TL, 1), F32)
    for k in [0] + order[::-1]:
        src = peer(k, -1)
        if k and (NX == 1 or k != NY):
            arrived(xg.at[src], rsem.at[0, k])
        xv = xg[src].astype(F32)
        ss = ss + jnp.sum(xv * xv, axis=-1, keepdims=True)
    scale = lax.rsqrt(ss / F32(SH * NT) + F32(1e-05))
    vcopy.wait()
    u = jnp.zeros((TL, 2 * HD), F32)
    for j in range(NT):
        xb = (xg[j].astype(F32) * scale).astype(BF)
        xn[j] = xb
        u = u + mm(xb, v[j * SH:(j + 1) * SH, :])
    u = u.astype(BF).astype(F32)

    ZP, DZ, Z0 = pl.ds(0, TL), pl.ds(TL, TL), pl.ds(2 * TL, TL)

    def gather_pass(part, phase):
        if NX > 1:
            src = peer(NY, -1)
            arrived(zc.at[src, part], rsem.at[phase, NY])
            for k in order:
                if k < NY:
                    pending.append(
                        send(
                            zc.at[src, part], zc.at[src, part], ssem.at[phase, NY + k], rsem.at[phase, NY + k],
                            (t, peer(k, 1)),
                        )
                    )

    def gather_start(part, phase, ks):
        for k in ks:
            pending.append(
                send(zc.at[d, part], zc.at[d, part], ssem.at[phase, k], rsem.at[phase, k], (t, peer(k, 1)))
            )

    zc[d, Z0, :] = mix(u).astype(BF)
    gather_start(Z0, 2, order)
    kacc = jnp.zeros((TL, TL), F32)
    for j in range(NT):
        kacc = kacc + mm_nt(xn[j], xn[j])
    kmat[...] = kacc.astype(BF)

    for k in order[::-1]:
        src = peer(k, -1)
        for i, (_, frm, lo, n) in enumerate(shares):
            arrived(osh.at[src, piece_of(frm, lo, n)], fsem.at[1, i, k])
        part = osh.at[src, pl.ds(c * HD, HD)]
        pending.append(send(part, part, fsem.at[0, 4, k], fsem.at[1, 4, k], (partner, d)))
    ocopy.wait()
    for k in order[::-1]:
        src = peer(k, -1)
        arrived(osh.at[src, pl.ds((1 - c) * HD, HD)], fsem.at[1, 4, k])

    GH = NT // 2
    RI = 2 * HD // NT
    mine_g = pl.ds(c * GH, GH)
    mine_r = pl.ds(z * RI, RI)
    rows = jnp.concatenate([osh[c * GH + g, mine_r, :] for g in range(GH)], axis=0)
    for k in order:
        p = peer(k, 1)
        gp_send[k] = mm_nt(rows, osh[p]).astype(BF)
        pending.append(send(gp_send.at[k], gp_recv.at[k], ssem.at[5, k], rsem.at[5, k], (t, p)))
    gram = mm_nt(rows, osh[d])

    NC = 4 if NT % 4 == 0 else 1
    CH = NT // NC

    def columns_start(part):
        for r in range(1, 4):
            send(
                xn.at[pl.ds(part * CH, CH), :, pl.ds(quad_il[r] * HD, HD)],
                xc.at[pl.ds(part * CH, CH), pl.ds(il * TL, TL), :],
                csem.at[0, r, part], csem.at[1, r, part], (quad[r], d),
            )

    acc = a0
    for k in [0] + order[::-1]:
        src = peer(k, -1)
        if k:
            arrived(zc.at[src, Z0], rsem.at[2, k])
        acc = acc + mm(zc[src, Z0, :], osh[src])
    err = (acc * s_w).astype(BF)
    a0b = a0.astype(BF)
    mixed = jnp.where(is_s, acc * s_w, a0).astype(BF)
    fer[1] = err
    for k in order:
        p = peer(k, 1)
        rs_send[k] = mm_nt(mixed, osh[p]).astype(BF)
        pending.append(send(rs_send.at[k], rs_recv.at[k], ssem.at[3, k], rsem.at[3, k], (t, p)))
    own = mm_nt(mixed, osh[d])
    for k in order[::-1]:
        arrived(gp_recv.at[k], rsem.at[5, k])
        gram = gram + gp_recv[k].astype(F32)
    for g in range(GH):
        gm[c * GH + g, mine_r, :] = gram[g * RI:(g + 1) * RI, :].astype(BF)
    zorder = sorted(range(1, NT), key=lambda k: -min(k, NT - k))
    for k in zorder:
        part = gm.at[mine_g, mine_r, :]
        pending.append(send(part, part, msem.at[0, k], msem.at[1, k], (zrot(k) * 4 + il, d)))
    xc[:, pl.ds(il * TL, TL), :] = xn[:, :, pl.ds(il * HD, HD)]
    ea = mm_nt(err, a0b)
    ee = mm_nt(err, err)
    for k in order[::-1]:
        arrived(rs_recv.at[k], rsem.at[3, k])
        own = own + rs_recv[k].astype(F32)
    dz = jnp.where(is_s, own, F32(0.0))
    a0o = jnp.where(is_s, F32(0.0), own)
    dzb = dz.astype(BF)
    u2 = u - RATE * mm(kmat[...], mix_t(dz).astype(BF))
    z2 = mix(u2).astype(BF)
    shares = jnp.concatenate([mm_nt(dzb, z2) + ea, ee], axis=1)
    zc[d, ZP, :] = jnp.where(is_s, shares, z2.astype(F32)).astype(BF)
    gather_start(ZP, 4, direct)
    gather_pass(ZP, 4)
    columns_start(0)
    if NC > 1:
        columns_start(1)
    for k in zorder:
        arrived(gm.at[mine_g, pl.ds(zback(k) * RI, RI), :], msem.at[1, k])
    pending.append(send(gm.at[mine_g], gm.at[mine_g], nsem.at[0], nsem.at[1], (partner, d)))
    arrived(gm.at[pl.ds((1 - c) * GH, GH)], nsem.at[1])

    zz = jnp.zeros((TL, TL), F32)
    tot = jnp.zeros((TL, 2 * HD), F32)
    fo = a0o
    for k in [0] + order[::-1]:
        src = peer(k, -1)
        if k and (NX == 1 or k != NY):
            arrived(zc.at[src, ZP], rsem.at[4, k])
        zp = zc[src, ZP, :]
        zz = zz + mm_nt(zp, zc[src, Z0, :])
        fo = fo + mm(zp, gm[src])
        tot = tot + zp.astype(F32)
    zzb = jnp.where(is_s, F32(0.0), RATE * zz).astype(BF)
    ef = jnp.where(is_s, tot[:, :TL], F32(0.0))
    eeb = jnp.where(is_s, tot[:, TL:], F32(0.0)).astype(BF)
    fet = (-RATE * q_row * (ef - mm_nt(eeb, zzb))).astype(BF)
    fo = q_w * (fo - mm(zzb, dzb))
    dz2 = fo + mm_tn(fet, zc[d, Z0, :])
    zc[d, DZ, :] = mix(-RATE * mm(kmat[...], mix_t(dz2).astype(BF))).astype(BF)
    gather_start(DZ, 6, direct)
    for part in range(2, NC):
        columns_start(part)
    acc = a0 - mm(zzb, fer[1])
    for j in range(NT):
        acc = acc + mm(zc[j, ZP, :], osh[j])
    fer[0] = (acc * q_w).astype(BF)
    acc = -mm_tn(zzb, fer[0])
    y_in = -mm_tn(zzb, fo.astype(BF))
    y_fix = mm(fet, z2)
    gather_pass(DZ, 6)
    for k in [0] + order[::-1]:
        src = peer(k, -1)
        if k and (NX == 1 or k != NY):
            arrived(zc.at[src, DZ], rsem.at[6, k])
        y_in = y_in + mm(zc[src, DZ, :], gm[src])
        acc = acc + mm(zc[src, DZ, :], osh[src])
    wall[pl.ds(il * TL, TL), :] = mix_t(dz2 + s_w * y_in + y_fix).astype(BF)
    for r in (3, 2, 1):
        mine = wall.at[pl.ds(il * TL, TL), :]
        pending.append(send(mine, mine, wsem.at[0, r], wsem.at[1, r], (quad[r], d)))

    fer[2] = (acc * s_w).astype(BF)
    errs = jnp.concatenate([fer[0], fer[1], fer[2]], axis=0)
    todo = order + [0]
    LAG = 4

    def piece(h):
        return pl.ds(h * (2 * HD // PH), 2 * HD // PH)

    def plane_start(h, rel, k):
        xt = xl + rel - 2 * rel * xl
        pending.append(
            send(
                xs_o.at[rel, k, piece(h)], xr_o.at[xl, d, piece(h)],
                hsem.at[h, rel, k], isem.at[h, xl, d], (z * 4 + xt * 2 + c, peer(k, 1)),
            )
        )

    for i in range(NT + LAG):
        if i < NT:
            j = peer(todo[i], 1)
            blk = mm_tn(zc[j], errs)
            for q in range(4):
                gob[q % 2, q // 2, j] = blk[:, q * HD:(q + 1) * HD].astype(BF)
            pending.append(
                send(gob.at[1 - c, :, j], cr_o.at[:, j], gsem.at[0, todo[i]], gsem.at[1, todo[i]], (partner, d))
            )
        if i >= LAG:
            k = todo[i - LAG]
            j = peer(k, 1)
            arrived(cr_o.at[:, j], gsem.at[1, k])
            for rel in (1, 0):
                xt = xl + rel - 2 * rel * xl
                tot = gob[c, xt, j].astype(F32) + cr_o[xt, j].astype(F32)
                if rel == 0 and k == 0:
                    xr_o[xl, d] = tot.astype(BF)
                else:
                    xs_o[rel, k] = tot.astype(BF)
                    plane_start(0, rel, k)
    for h in range(1, PH):
        for k in todo:
            for rel in (1, 0):
                if rel or k:
                    plane_start(h, rel, k)

    for part in range(NC):
        for r in range(1, 4):
            arrived(xc.at[pl.ds(part * CH, CH), pl.ds(quad_il[r] * TL, TL), :], csem.at[1, r, part])
    for r in range(1, 4):
        arrived(wall.at[pl.ds(quad_il[r] * TL, TL), :], wsem.at[1, r])
    DN = NT // 2
    UP = NT - 1 - DN

    def v_block(zt):
        return mm_tn(xc[zt], wall[...])

    def ring(way, hop, total):
        to = zback(1) if way == 0 else zrot(1)
        zs_v[way, hop] = total.astype(BF)
        pending.append(
            send(
                zs_v.at[way, hop], zr_v.at[way, hop], psem.at[way, hop], qsem.at[way, hop], (to * 4 + il, d)
            )
        )

    def ring_first():
        ring(0, 0, v_block(zback(DN)))
        if UP:
            ring(1, 0, v_block(zrot(UP)))

    def ring_next(hop):
        for way, count in ((0, DN), (1, UP)):
            if hop < count:
                blk = v_block(zback(DN - hop) if way == 0 else zrot(UP - hop))
                arrived(zr_v.at[way, hop - 1], qsem.at[way, hop - 1])
                ring(way, hop, blk + zr_v[way, hop - 1].astype(F32))

    def plane_o(h, k):
        zt = zrot(k)
        for xs in range(2):

            @pl.when((xl != xs) | (d != zt))
            def _():
                arrived(xr_o.at[xs, zt, piece(h)], isem.at[h, xs, zt])

        tot = xr_o[0, zt, piece(h)].astype(F32) + xr_o[1, zt, piece(h)].astype(F32)
        if k:
            zs_o[k, piece(h)] = tot.astype(BF)
            pending.append(
                send(
                    zs_o.at[k, piece(h)], zr_o.at[k, piece(h)], tsem.at[0, h, k], tsem.at[1, h, k],
                    (zt * 4 + il, d),
                )
            )
        return tot

    ring_first()
    own_o = []
    if DN > 1:
        ring_next(1)
    if DN > 2:
        ring_next(2)
    for k in zorder + [0]:
        tot = plane_o(0, k)
    own_o.append(tot)
    for k in zorder + [0]:
        tot = plane_o(1, k)
    own_o.append(tot)
    if DN > 3:
        ring_next(3)
    own_v = v_block(z)
    for way, count in ((0, DN), (1, UP)):
        if count:
            arrived(zr_v.at[way, count - 1], qsem.at[way, count - 1])
            own_v = own_v + zr_v[way, count - 1].astype(F32)
    out_v[...] = own_v
    for h in range(PH):
        tot = own_o[h]
        for k in zorder[::-1]:
            arrived(zr_o.at[k, piece(h)], tsem.at[1, h, k])
            tot = tot + zr_o[k, piece(h)].astype(F32)
        out_o[piece(h), :] = tot

    for cp in pending:
        cp.wait_send()
    for r in range(1, 4):
        for part in range(NC):
            sent(xc.at[pl.ds(0, CH), pl.ds(0, TL), :], csem.at[0, r, part])


def per_device(inputs, targets, queries, key_rows, value_weight, output_weight, splits, *, NT):
    NX = 2 if NT % 8 == 0 else 1
    NY = NT // NX
    SH = inputs.shape[1]
    vm = pltpu.VMEM
    vspec = pl.BlockSpec(memory_space=pltpu.VMEM)
    aspec = pl.BlockSpec(memory_space=pl.ANY)
    dma = pltpu.SemaphoreType.DMA
    parts = pl.pallas_call(
        functools.partial(body, NT, NX, NY),
        out_shape=(pltpu.VMEM((TL, 2 * HD), F32), pltpu.VMEM((2 * HD, TL), F32)),
        in_specs=[aspec] * 6 + [pl.BlockSpec(memory_space=pltpu.SMEM)],
        out_specs=(vspec, vspec),
        scratch_shapes=[
            vm((SH * NT, 2 * HD), BF),
            vm((NT, TL, SH), BF),
            vm((NT, TL, SH), BF),
            vm((NT, 2 * HD, SH), BF),
            vm((NT, 3 * TL, 2 * HD), BF),
            vm((3, TL, SH), BF),
            vm((NT, TL, 2 * HD), BF),
            vm((NT, TL, 2 * HD), BF),
            vm((TL, TL), BF),
            vm((2, TL, TL), BF),
            vm((2, 2, NT, 2 * HD, HD), BF),
            vm((2, NT, 2 * HD, HD), BF),
            vm((2, NT, 2 * HD, HD), BF),
            vm((2, NT, 2 * HD, HD), BF),
            vm((NT, 2 * HD, HD), BF),
            vm((NT, 2 * HD, HD), BF),
            vm((NT, 4 * TL, HD), BF),
            vm((4 * TL, 2 * HD), BF),
            vm((2, NT // 2, TL, 2 * HD), BF),
            vm((2, NT // 2, TL, 2 * HD), BF),
            vm((NT, TL, 2 * HD), BF),
            vm((NT, TL, 2 * HD), BF),
            vm((NT, 2 * HD, 2 * HD), BF),
            vm((TL, SH), BF),
            vm((TL, 2 * HD), BF),
            vm((TL, 2 * HD), BF),
            dma((6,)),
            dma((8, NT)),
            dma((8, NT)),
            dma((2, 5, NT)),
            dma((2, NT)),
            dma((PH, 2, NT)),
            dma((PH, 2, NT)),
            dma((2, 4)),
            dma((2, 4, 4)),
            dma((2, NT)),
            dma((2, NT)),
            dma((2, NT)),
            dma((4,)),
            dma((2, PH, NT)),
        ],
        compiler_params=pltpu.CompilerParams(
            collective_id=0, has_side_effects=True, vmem_limit_bytes=60 * 1024 * 1024
        ),
        name="meta",
    )(inputs, targets, queries, key_rows, value_weight, output_weight, splits)
    return parts


def solution(mesh):
    return jax.shard_map(
        functools.partial(per_device, NT=mesh.shape["tensor"]),
        mesh=mesh,
        in_specs=(
            P("task", "tensor"),
            P("task", "tensor"),
            P("task", "tensor"),
            P("task", "tensor"),
            P(None, "tensor"),
            P("tensor", None),
            P("task"),
        ),
        out_specs=(P("task", "tensor"), P("tensor", "task")),
        check_vma=False,
    )
```
